16 devices in a mesh: dp: 4 (over z, y), dcp: 4 (over x, core).
Axes of the slice: x: 2, y: 2, z: 2, core: 2. Of those that a mesh axis runs over, the one named last changes fastest.
Arguments:
- q_abs: bfloat16 [128, 64, 576], P('dp', 'dcp'), parts along dimension 0
- cache: bfloat16 [128, 8192, 576], P('dp', 'dcp'), parts along dimension 0
- lengths: int32 [128], P('dp'), parts along dimension 0
Outputs:
- output: bfloat16 [128, 64, 512], P('dp', 'dcp'), parts along dimension 0
There are 4 independent parts. The reference program is written for one: setup_inputs(seed, part) draws one part's arguments, and reference() takes and returns one part's arrays. A program takes and returns all parts, laid end to end along the dimension named above; each array names one.
All inputs are finite; a program needn't handle non-finite values.
Results may differ from the reference program's by a relative error of at most 0.00673794.
Values are sent between devices in bfloat16 or wider.
A program may use at most 1 GiB of HBM per device.

```python
import jax
import jax.numpy as jnp
from jax import lax

HEADS = 64
KV_RANK = 512
ROPE = 64
QK_NOPE = 128
B = 32
S = 8192
NDEV = 4

WIDTH = KV_RANK + ROPE
SCALE = (QK_NOPE + ROPE) ** -0.5
BLOCK = S // NDEV
SEG = S // 32


def setup_inputs(seed: int = 0, part: int = 0) -> dict:
    key = jax.random.fold_in(jax.random.key(seed), part)
    kq, kc, kf, ks = jax.random.split(key, 4)
    q_abs = (jax.random.normal(kq, (B, HEADS, WIDTH), jnp.float32) * 0.6).astype(jnp.bfloat16)

    def draw(k):
        k1, k2, k3 = jax.random.split(k, 3)
        seg = jax.random.normal(k1, (32, KV_RANK), jnp.float32)
        lat = jax.random.normal(k2, (S, KV_RANK), jnp.float32) + jnp.repeat(seg, SEG, axis=0)
        rope = jax.random.normal(k3, (S, ROPE), jnp.float32) * 3.0
        return jnp.concatenate([lat, rope], axis=1).astype(jnp.bfloat16)

    cache = lax.map(draw, jax.random.split(kc, B))
    full = S - jax.random.randint(kf, (B,), 0, S // 64)
    short = jax.random.randint(ks, (B,), 1, S + 1)
    lengths = jnp.where(jnp.arange(B) % 2 == 0, full, short).astype(jnp.int32)
    return {'q_abs': q_abs, 'cache': cache, 'lengths': lengths}


def reference(q_abs, cache, lengths):
    pos = jnp.arange(S).reshape(NDEV, BLOCK)

    def one(args):
        qb, cb, lb = args
        cf = cb.astype(jnp.float32).reshape(NDEV, BLOCK, WIDTH)
        s = jnp.einsum('hk,ntk->nht', qb.astype(jnp.float32), cf) * SCALE
        valid = pos < lb
        s = jnp.where(valid[:, None, :], s, -jnp.inf)
        m = jnp.max(s, axis=2)
        m0 = jnp.where(jnp.isfinite(m), m, 0.0)
        p = jnp.exp(s - m0[:, :, None])
        l = jnp.sum(p, axis=2)
        pb = p.astype(jnp.bfloat16).astype(jnp.float32)
        pv = jnp.einsum('nht,ntc->nhc', pb, cf[:, :, :KV_RANK])
        has = l > 0.0
        l1 = jnp.where(has, l, 1.0)
        od = (pv / l1[:, :, None]).astype(jnp.bfloat16).astype(jnp.float32)
        lse_d = jnp.where(has, m0 + jnp.log(l1), -jnp.inf)
        mx = jnp.max(lse_d, axis=0)
        lse = mx + jnp.log(jnp.sum(jnp.exp(lse_d - mx[None, :]), axis=0))
        o = jnp.sum(jnp.exp(lse_d - lse[None, :])[:, :, None] * od, axis=0)
        return o.astype(jnp.bfloat16)

    return lax.map(one, (q_abs, cache, lengths))
```

```python
import functools

import jax
import jax.numpy as jnp
from jax import lax
from jax.experimental import pallas as pl
from jax.experimental.pallas import tpu as pltpu
from jax.sharding import PartitionSpec as P

ROPE = 64
SCALE = 192 ** -0.5
LOG2E = 1.4426950408889634
SLOTS = 8


def kernel(len_ref, q_ref, cache_ref, out_ref, cbuf, qbuf, s_a, s_b, mx_a, mx_b, obuf, orecv, lbuf, lrecv,
           c_sem, q_sem, qs_sem, qr_sem, os_sem, or_sem, ls_sem, lr_sem):
    nb, heads, wd = qbuf.shape
    own = q_ref.shape[1]
    lat = wd - ROPE
    sl = cbuf.shape[2]
    pairs = nb // 2
    g = lax.axis_index('dp')
    d = lax.axis_index('dcp')
    mate = d + 1 - 2 * (d % 2)
    over = (d + 2) % 4
    far = mate + 2 - 4 * (mate // 2)
    peers = (mate, over, far)

    def rows(j):
        return pl.ds(pl.multiple_of(j * own, own), own)

    def cache_copy(b):
        slot = b % SLOTS
        return pltpu.make_async_copy(cache_ref.at[b], cbuf.at[slot], c_sem.at[slot])

    def remote(src, dst, ssem, rsem, dev):
        return pltpu.make_async_remote_copy(src_ref=src, dst_ref=dst, send_sem=ssem, recv_sem=rsem,
                                            device_id=(g, dev), device_id_type=pl.DeviceIdType.MESH)

    def q_copy(kind, c, src_dev, to):
        view = qbuf.at[pl.ds(2 * c, 2), rows(src_dev), :]
        return remote(view, view, qs_sem.at[kind, c], qr_sem.at[kind, c], to)

    def o_copy(i, b, src_dev, dst_dev):
        return remote(obuf.at[b, rows(dst_dev), :], orecv.at[src_dev, b], os_sem.at[i, b], or_sem.at[i, b], dst_dev)

    def l_copy(i, src_dev, dst_dev):
        return remote(lbuf.at[rows(dst_dev), :], lrecv.at[src_dev], ls_sem.at[i], lr_sem.at[i], dst_dev)

    q_own = pltpu.make_async_copy(q_ref, qbuf.at[:, rows(d), :], q_sem)
    q_own.start()
    for b in range(6):
        cache_copy(b).start()

    barrier = pltpu.get_barrier_semaphore()
    for p in peers:
        pl.semaphore_signal(barrier, inc=1, device_id=(g, p), device_id_type=pl.DeviceIdType.MESH)
    pl.semaphore_wait(barrier, 3)

    q_own.wait()

    def send_q(c, _):
        q_copy(1, c, d, over).start()
        q_copy(0, c, d, mate).start()
        return 0

    lax.fori_loop(0, pairs, send_q, 0)

    def forward_q(c):
        q_copy(1, c, over, over).wait_recv()
        q_copy(2, c, over, mate).start()

    def wait_q(c):
        q_copy(0, c, mate, mate).wait_recv()
        q_copy(2, c, far, mate).wait_recv()

    def send_o(b):
        for i in (1, 2, 0):
            o_copy(i, b, d, peers[i]).start()

    def scores(b, s_ref, mx_ref):
        n_valid = len_ref[b] - d * sl
        c = cbuf.at[b % SLOTS]
        s = jnp.dot(qbuf[b], c[...], preferred_element_type=jnp.float32)
        pos = lax.broadcasted_iota(jnp.int32, s.shape, 1)
        s = jnp.where(pos < n_valid, s, -jnp.inf)
        s_ref[...] = s
        mx = s[:, :128]
        for k in range(1, sl // 128):
            mx = jnp.maximum(mx, s[:, 128 * k:128 * (k + 1)])
        mx_ref[...] = mx

    def values(b, s_ref, mx_ref):
        c = cbuf.at[b % SLOTS]
        m = jnp.max(mx_ref[...], axis=1, keepdims=True)
        m0 = jnp.where(m == -jnp.inf, 0.0, m)
        p = jnp.exp2((s_ref[...] - m0) * (SCALE * LOG2E))
        l = jnp.sum(p, axis=1, keepdims=True)
        pv = lax.dot_general(p.astype(jnp.bfloat16), c[:lat, :], (((1,), (1,)), ((), ())), preferred_element_type=jnp.float32)
        has = l > 0.0
        l1 = jnp.where(has, l, 1.0)
        obuf[b] = (pv * (1.0 / l1)).astype(jnp.bfloat16)
        lse = jnp.where(has, m0 * SCALE + jnp.log(l1), -jnp.inf)
        lane = lax.broadcasted_iota(jnp.int32, lbuf.shape, 1)
        lbuf[...] = jnp.where(lane == b, lse, lbuf[...])

    lbuf[...] = jnp.zeros_like(lbuf)
    forward_q(0)
    forward_q(1)
    wait_q(0)
    cache_copy(0).wait()
    cache_copy(1).wait()
    scores(0, s_a, mx_a)
    scores(1, s_b, mx_b)
    values(0, s_a, mx_a)

    def body(k, _):
        @pl.when(k < pairs - 1)
        def _():
            forward_q(k + 1)

        wait_q(k)

        @pl.when(k < pairs - 2)
        def _():
            cache_copy(2 * k + 4).start()
            cache_copy(2 * k + 5).start()

        @pl.when(k > 1)
        def _():
            send_o(2 * k - 3)

        send_o(2 * k - 2)
        cache_copy(2 * k).wait()
        cache_copy(2 * k + 1).wait()
        scores(2 * k, s_a, mx_a)
        values(2 * k - 1, s_b, mx_b)
        scores(2 * k + 1, s_b, mx_b)
        values(2 * k, s_a, mx_a)
        return 0

    lax.fori_loop(1, pairs, body, 0)
    send_o(nb - 3)
    send_o(nb - 2)
    values(nb - 1, s_b, mx_b)
    for i in (1, 2, 0):
        l_copy(i, d, peers[i]).start()
    send_o(nb - 1)

    for i in (0, 1, 2):
        l_copy(i, peers[i], d).wait_recv()
    lses = [lbuf[rows(d), :]] + [lrecv[p] for p in peers]
    top = functools.reduce(jnp.maximum, lses)
    wts = [jnp.exp(x - top) for x in lses]
    norm = 1.0 / functools.reduce(jnp.add, wts)
    wts = [x * norm for x in wts]
    lane = lax.broadcasted_iota(jnp.int32, wts[0].shape, 1)

    def merge(k, _):
        for b in (2 * k, 2 * k + 1):
            for i in (0, 1, 2):
                o_copy(i, b, peers[i], d).wait_recv()
        for b in (2 * k, 2 * k + 1):
            parts = [obuf[b, rows(d), :]] + [orecv[p, b] for p in peers]
            total = None
            for w, o in zip(wts, parts):
                col = jnp.sum(jnp.where(lane == b, w, 0.0), axis=1, keepdims=True)
                term = col * o.astype(jnp.float32)
                total = term if total is None else total + term
            out_ref[b] = total.astype(jnp.bfloat16)
        return 0

    lax.fori_loop(0, pairs, merge, 0)

    for i in (0, 1, 2):
        l_copy(i, d, peers[i]).wait_send()

    def drain(b, _):
        for i in (0, 1, 2):
            o_copy(i, b, d, peers[i]).wait_send()
        return 0

    lax.fori_loop(0, nb, drain, 0)

    def drain_q(c, _):
        q_copy(0, c, d, mate).wait_send()
        q_copy(1, c, d, over).wait_send()
        q_copy(2, c, over, mate).wait_send()
        return 0

    lax.fori_loop(0, pairs, drain_q, 0)


def solution(mesh):
    n = mesh.shape['dcp']

    def local(q, cache, lengths):
        b, own, wd = q.shape
        sl = cache.shape[1]
        lat = wd - ROPE
        heads = own * n
        vmem = pl.BlockSpec(memory_space=pltpu.VMEM)
        return pl.pallas_call(
            kernel,
            out_shape=jax.ShapeDtypeStruct((b, own, lat), jnp.bfloat16),
            in_specs=[
                pl.BlockSpec(memory_space=pltpu.SMEM),
                pl.BlockSpec(memory_space=pl.ANY),
                pl.BlockSpec(memory_space=pl.ANY),
            ],
            out_specs=vmem,
            scratch_shapes=[
                pltpu.VMEM((SLOTS, wd, sl), jnp.bfloat16),
                pltpu.VMEM((b, heads, wd), jnp.bfloat16),
                pltpu.VMEM((heads, sl), jnp.float32),
                pltpu.VMEM((heads, sl), jnp.float32),
                pltpu.VMEM((heads, 128), jnp.float32),
                pltpu.VMEM((heads, 128), jnp.float32),
                pltpu.VMEM((b, heads, lat), jnp.bfloat16),
                pltpu.VMEM((n, b, own, lat), jnp.bfloat16),
                pltpu.VMEM((heads, 128), jnp.float32),
                pltpu.VMEM((n, own, 128), jnp.float32),
                pltpu.SemaphoreType.DMA((SLOTS,)),
                pltpu.SemaphoreType.DMA,
                pltpu.SemaphoreType.DMA((3, b // 2)),
                pltpu.SemaphoreType.DMA((3, b // 2)),
                pltpu.SemaphoreType.DMA((3, b)),
                pltpu.SemaphoreType.DMA((3, b)),
                pltpu.SemaphoreType.DMA((3,)),
                pltpu.SemaphoreType.DMA((3,)),
            ],
            compiler_params=pltpu.CompilerParams(
                collective_id=0, has_side_effects=True, vmem_limit_bytes=56 * 2 ** 20
            ),
            name='mla_decode',
        )(lengths, q, jnp.swapaxes(cache, 1, 2))

    return jax.shard_map(local, mesh=mesh, in_specs=(P('dp', 'dcp', None), P('dp', 'dcp', None), P('dp')), out_specs=P('dp', 'dcp', None), check_vma=False)
```

```python
import functools

import jax
import jax.numpy as jnp
from jax import lax
from jax.experimental import pallas as pl
from jax.experimental.pallas import tpu as pltpu
from jax.sharding import PartitionSpec as P

ROPE = 64
SCALE = 192 ** -0.5
LOG2E = 1.4426950408889634
SLOTS = 8
LEAD = 4
NT = (((1,), (1,)), ((), ()))


def kernel(len_ref, q_ref, cache_ref, out_ref, cbuf, qbuf, s_a, s_b, mx_a, mx_b, obuf, orecv, lbuf, lrecv,
           c_sem, q_sem, ms_sem, mr_sem, qs_sem, qr_sem, os_sem, or_sem, ls_sem, lr_sem):
    nb, heads, wd = qbuf.shape
    own = q_ref.shape[1]
    lat = wd - ROPE
    sl = cbuf.shape[2]
    pairs = nb // 2
    g = lax.axis_index('dp')
    d = lax.axis_index('dcp')
    mate = d + 1 - 2 * (d % 2)
    over = (d + 2) % 4
    far = mate + 2 - 4 * (mate // 2)
    peers = (mate, over, far)

    def rows(j):
        return pl.ds(pl.multiple_of(j * own, own), own)

    def cache_copy(b):
        slot = b % SLOTS
        return pltpu.make_async_copy(cache_ref.at[b], cbuf.at[slot], c_sem.at[slot])

    def remote(src, dst, ssem, rsem, dev):
        return pltpu.make_async_remote_copy(src_ref=src, dst_ref=dst, send_sem=ssem, recv_sem=rsem,
                                            device_id=(g, dev), device_id_type=pl.DeviceIdType.MESH)

    def mate_copy(i, src_dev, to):
        view = qbuf.at[pl.ds(0, 2) if i == 0 else pl.ds(2, nb - 2), rows(src_dev), :]
        return remote(view, view, ms_sem.at[i], mr_sem.at[i], to)

    def q_copy(kind, c, src_dev, to):
        view = qbuf.at[pl.ds(2 * c, 2), rows(src_dev), :]
        return remote(view, view, qs_sem.at[kind, c], qr_sem.at[kind, c], to)

    def o_copy(i, b, src_dev, dst_dev):
        return remote(obuf.at[b, rows(dst_dev), :], orecv.at[src_dev, b], os_sem.at[i, b], or_sem.at[i, b], dst_dev)

    def l_copy(t, i, src_dev, dst_dev):
        return remote(lbuf.at[t, rows(dst_dev), :], lrecv.at[t, src_dev], ls_sem.at[t, i], lr_sem.at[t, i], dst_dev)

    q_own = pltpu.make_async_copy(q_ref, qbuf.at[:, rows(d), :], q_sem)
    q_own.start()

    barrier = pltpu.get_barrier_semaphore()
    for p in peers:
        pl.semaphore_signal(barrier, inc=1, device_id=(g, p), device_id_type=pl.DeviceIdType.MESH)
    pl.semaphore_wait(barrier, 3)

    q_own.wait()
    q_copy(0, 0, d, over).start()
    mate_copy(0, d, mate).start()
    cache_copy(0).start()
    cache_copy(1).start()
    for c in range(1, LEAD):
        q_copy(0, c, d, over).start()
    mate_copy(1, d, mate).start()
    for b in range(2, 6):
        cache_copy(b).start()

    def forward_q(c):
        q_copy(0, c, over, over).wait_recv()
        q_copy(1, c, over, mate).start()

    def wait_q(c):
        q_copy(1, c, far, mate).wait_recv()

    def send_o(b):
        for i in (1, 2, 0):
            o_copy(i, b, d, peers[i]).start()

    def scores(b, s_ref, j, w, top):
        n_valid = len_ref[b] - d * sl
        c = cbuf.at[b % SLOTS]
        s = jnp.dot(qbuf[b], c[:, w * j:w * (j + 1)], preferred_element_type=jnp.float32)
        pos = lax.broadcasted_iota(jnp.int32, s.shape, 1) + w * j
        s = jnp.where(pos < n_valid, s, -jnp.inf)
        s_ref[:, w * j:w * (j + 1)] = s
        for k in range(w // 128):
            t = s[:, 128 * k:128 * (k + 1)]
            top = t if top is None else jnp.maximum(top, t)
        return top

    def weights(b, s_ref, mx_ref, src, dst):
        m = jnp.max(mx_ref[...], axis=1, keepdims=True)
        m0 = jnp.where(m == -jnp.inf, 0.0, m)
        p = jnp.exp2((s_ref[...] - m0) * (SCALE * LOG2E))
        l = jnp.sum(p, axis=1, keepdims=True)
        has = l > 0.0
        l1 = jnp.where(has, l, 1.0)
        lse = jnp.where(has, m0 * SCALE + jnp.log(l1), -jnp.inf)
        lane = lax.broadcasted_iota(jnp.int32, lbuf.shape[1:], 1)
        lbuf[dst] = jnp.where(lane == b, lse, lbuf[src])
        return p.astype(jnp.bfloat16), 1.0 / l1

    def values(b, pb, inv, m, w):
        c = cbuf.at[b % SLOTS]
        t = lax.dot_general(c[w * m:w * (m + 1), :], pb, NT, preferred_element_type=jnp.float32)
        obuf[b, :, w * m:w * (m + 1)] = (t.T * inv).astype(jnp.bfloat16)

    def step(bq, sq, mxq, bv, sv, mxv):
        if bv is not None:
            pb, inv = weights(bv, sv, mxv, 0, 0)
        top = None
        for j in range(8):
            top = scores(bq, sq, j, sl // 8, top)
            if bv is not None and j % 2 == 1:
                values(bv, pb, inv, j // 2, lat // 4)
        mxq[...] = top

    lbuf[0] = jnp.zeros(lbuf.shape[1:], jnp.float32)
    forward_q(0)
    mate_copy(0, mate, mate).wait_recv()
    cache_copy(0).wait()
    cache_copy(1).wait()
    forward_q(1)
    wait_q(0)
    step(0, s_a, mx_a, None, None, None)
    step(1, s_b, mx_b, 0, s_a, mx_a)
    mate_copy(1, mate, mate).wait_recv()

    def body(k, _):
        @pl.when(k < pairs - 1)
        def _():
            forward_q(k + 1)

        wait_q(k)

        @pl.when(k < pairs - LEAD + 1)
        def _():
            q_copy(0, k + LEAD - 1, d, over).start()

        @pl.when(k < pairs - 2)
        def _():
            cache_copy(2 * k + 4).start()
            cache_copy(2 * k + 5).start()

        @pl.when(k > 1)
        def _():
            send_o(2 * k - 3)

        send_o(2 * k - 2)
        cache_copy(2 * k).wait()
        cache_copy(2 * k + 1).wait()
        step(2 * k, s_a, mx_a, 2 * k - 1, s_b, mx_b)
        step(2 * k + 1, s_b, mx_b, 2 * k, s_a, mx_a)
        return 0

    lax.fori_loop(1, pairs, body, 0)

    def send_l(t):
        for i in (1, 2, 0):
            l_copy(t, i, d, peers[i]).start()

    send_o(nb - 3)
    send_o(nb - 2)
    send_l(0)
    pb, inv = weights(nb - 1, s_b, mx_b, 0, 1)
    for m in range(4):
        values(nb - 1, pb, inv, m, lat // 4)
    send_o(nb - 1)
    send_l(1)

    def shares(t):
        for i in (0, 1, 2):
            l_copy(t, i, peers[i], d).wait_recv()
        lses = [lbuf[t, rows(d), :]] + [lrecv[t, p] for p in peers]
        top = functools.reduce(jnp.maximum, lses)
        ws = [jnp.exp(x - top) for x in lses]
        norm = 1.0 / functools.reduce(jnp.add, ws)
        return [x * norm for x in ws]

    def merge(ws, b0):
        for b in (b0, b0 + 1):
            for i in (0, 1, 2):
                o_copy(i, b, peers[i], d).wait_recv()
        lane = lax.broadcasted_iota(jnp.int32, ws[0].shape, 1)
        for b in (b0, b0 + 1):
            parts = [obuf[b, rows(d), :]] + [orecv[p, b] for p in peers]
            total = None
            for w, o in zip(ws, parts):
                col = jnp.sum(jnp.where(lane == b, w, 0.0), axis=1, keepdims=True)
                term = col * o.astype(jnp.float32)
                total = term if total is None else total + term
            out_ref[b] = total.astype(jnp.bfloat16)

    early = shares(0)

    def merge_early(k, _):
        merge(early, 2 * k)
        return 0

    lax.fori_loop(0, pairs - 1, merge_early, 0)
    merge(shares(1), nb - 2)

    for t in (0, 1):
        for i in (0, 1, 2):
            l_copy(t, i, d, peers[i]).wait_send()
    for i in (0, 1):
        mate_copy(i, d, mate).wait_send()

    def drain(b, _):
        for i in (0, 1, 2):
            o_copy(i, b, d, peers[i]).wait_send()
        return 0

    lax.fori_loop(0, nb, drain, 0)

    def drain_q(c, _):
        q_copy(0, c, d, over).wait_send()
        q_copy(1, c, over, mate).wait_send()
        return 0

    lax.fori_loop(0, pairs, drain_q, 0)


def solution(mesh):
    n = mesh.shape['dcp']

    def local(q, cache, lengths):
        b, own, wd = q.shape
        sl = cache.shape[1]
        lat = wd - ROPE
        heads = own * n
        vmem = pl.BlockSpec(memory_space=pltpu.VMEM)
        return pl.pallas_call(
            kernel,
            out_shape=jax.ShapeDtypeStruct((b, own, lat), jnp.bfloat16),
            in_specs=[
                pl.BlockSpec(memory_space=pltpu.SMEM),
                pl.BlockSpec(memory_space=pltpu.HBM),
                pl.BlockSpec(memory_space=pltpu.HBM),
            ],
            out_specs=vmem,
            scratch_shapes=[
                pltpu.VMEM((SLOTS, wd, sl), jnp.bfloat16),
                pltpu.VMEM((b, heads, wd), jnp.bfloat16),
                pltpu.VMEM((heads, sl), jnp.float32),
                pltpu.VMEM((heads, sl), jnp.float32),
                pltpu.VMEM((heads, 128), jnp.float32),
                pltpu.VMEM((heads, 128), jnp.float32),
                pltpu.VMEM((b, heads, lat), jnp.bfloat16),
                pltpu.VMEM((n, b, own, lat), jnp.bfloat16),
                pltpu.VMEM((2, heads, 128), jnp.float32),
                pltpu.VMEM((2, n, own, 128), jnp.float32),
                pltpu.SemaphoreType.DMA((SLOTS,)),
                pltpu.SemaphoreType.DMA,
                pltpu.SemaphoreType.DMA((2,)),
                pltpu.SemaphoreType.DMA((2,)),
                pltpu.SemaphoreType.DMA((2, b // 2)),
                pltpu.SemaphoreType.DMA((2, b // 2)),
                pltpu.SemaphoreType.DMA((3, b)),
                pltpu.SemaphoreType.DMA((3, b)),
                pltpu.SemaphoreType.DMA((2, 3)),
                pltpu.SemaphoreType.DMA((2, 3)),
            ],
            compiler_params=pltpu.CompilerParams(
                collective_id=0, has_side_effects=True, vmem_limit_bytes=40 * 2 ** 20
            ),
            name='mla_decode',
        )(lengths, q, jnp.swapaxes(cache, 1, 2))

    return jax.shard_map(local, mesh=mesh, in_specs=(P('dp', 'dcp', None), P('dp', 'dcp', None), P('dp')), out_specs=P('dp', 'dcp', None), check_vma=False)
```

```python
import functools

import jax
import jax.numpy as jnp
from jax import lax
from jax.experimental import pallas as pl
from jax.experimental.pallas import tpu as pltpu
from jax.sharding import PartitionSpec as P

ROPE = 64
SCALE = 192 ** -0.5
LOG2E = 1.4426950408889634
SLOTS = 8
LEAD = 5
NT = (((1,), (1,)), ((), ()))


def kernel(lens_ref, q_ref, cache_ref, out_ref, cbuf, qbuf, s_a, s_b, mx_a, mx_b, obuf, orecv, lbuf, lrecv, len_ref,
           n_sem, c_sem, q_sem, ms_sem, mr_sem, qs_sem, qr_sem, os_sem, or_sem, ls_sem, lr_sem):
    nb, heads, wd = qbuf.shape
    own = q_ref.shape[1]
    lat = wd - ROPE
    sl = cbuf.shape[2]
    pairs = nb // 2
    g = lax.axis_index('dp')
    d = lax.axis_index('dcp')
    mate = d + 1 - 2 * (d % 2)
    over = (d + 2) % 4
    far = mate + 2 - 4 * (mate // 2)
    peers = (mate, over, far)

    def rows(j):
        return pl.ds(pl.multiple_of(j * own, own), own)

    def cache_copy(b):
        slot = b % SLOTS
        return pltpu.make_async_copy(cache_ref.at[b], cbuf.at[slot], c_sem.at[slot])

    def remote(src, dst, ssem, rsem, dev):
        return pltpu.make_async_remote_copy(src_ref=src, dst_ref=dst, send_sem=ssem, recv_sem=rsem,
                                            device_id=(g, dev), device_id_type=pl.DeviceIdType.MESH)

    def mate_copy(i, src_dev, to):
        view = qbuf.at[pl.ds(0, 2) if i == 0 else pl.ds(2, nb - 2), rows(src_dev), :]
        return remote(view, view, ms_sem.at[i], mr_sem.at[i], to)

    def q_copy(kind, c, src_dev, to):
        view = qbuf.at[pl.ds(2 * c, 2), rows(src_dev), :]
        return remote(view, view, qs_sem.at[kind, c], qr_sem.at[kind, c], to)

    def o_copy(i, c, src_dev, dst_dev):
        if isinstance(c, int) and c in (0, pairs):
            at = pl.ds(1, 1) if c == 0 else pl.ds(nb, 1)
        else:
            at = pl.ds(2 * c, 2)
        return remote(obuf.at[at, rows(dst_dev), :], orecv.at[src_dev, at], os_sem.at[i, c], or_sem.at[i, c], dst_dev)

    def l_copy(t, i, src_dev, dst_dev):
        return remote(lbuf.at[t, rows(dst_dev), :], lrecv.at[t, src_dev], ls_sem.at[t, i], lr_sem.at[t, i], dst_dev)

    q_own = pltpu.make_async_copy(q_ref, qbuf.at[:, rows(d), :], q_sem)
    q_own.start()
    lens = pltpu.make_async_copy(lens_ref, len_ref, n_sem)
    lens.start()
    cache_copy(0).start()
    cache_copy(1).start()

    barrier = pltpu.get_barrier_semaphore()
    for p in peers:
        pl.semaphore_signal(barrier, inc=1, device_id=(g, p), device_id_type=pl.DeviceIdType.MESH)
    pl.semaphore_wait(barrier, 3)

    q_own.wait()
    q_copy(0, 0, d, over).start()
    mate_copy(0, d, mate).start()
    for c in range(1, LEAD):
        q_copy(0, c, d, over).start()
    mate_copy(1, d, mate).start()
    for b in range(2, 6):
        cache_copy(b).start()

    def forward_q(c):
        q_copy(0, c, over, over).wait_recv()
        q_copy(1, c, over, mate).start()

    def wait_q(c):
        q_copy(1, c, far, mate).wait_recv()

    def send_o(c):
        for i in (1, 2, 0):
            o_copy(i, c, d, peers[i]).start()

    def wait_o(c):
        for i in (0, 1, 2):
            o_copy(i, c, peers[i], d).wait_recv()

    def scores(b, s_ref, j, w, top):
        n_valid = len_ref[b] - d * sl
        c = cbuf.at[b % SLOTS]
        s = jnp.dot(qbuf[b], c[:, w * j:w * (j + 1)], preferred_element_type=jnp.float32)
        pos = lax.broadcasted_iota(jnp.int32, s.shape, 1) + w * j
        s = jnp.where(pos < n_valid, s, -jnp.inf)
        s_ref[:, w * j:w * (j + 1)] = s
        for k in range(w // 128):
            t = s[:, 128 * k:128 * (k + 1)]
            top = t if top is None else jnp.maximum(top, t)
        return top

    def weights(b, s_ref, mx_ref, src, dst):
        m = jnp.max(mx_ref[...], axis=1, keepdims=True)
        m0 = jnp.where(m == -jnp.inf, 0.0, m)
        p = jnp.exp2((s_ref[...] - m0) * (SCALE * LOG2E))
        l = jnp.sum(p, axis=1, keepdims=True)
        has = l > 0.0
        l1 = jnp.where(has, l, 1.0)
        lse = jnp.where(has, m0 * SCALE + jnp.log(l1), -jnp.inf)
        lane = lax.broadcasted_iota(jnp.int32, lbuf.shape[1:], 1)
        lbuf[dst] = jnp.where(lane == b, lse, lbuf[src])
        return p.astype(jnp.bfloat16), 1.0 / l1

    def step(bq, sq, mxq, bv, sv, mxv, dst=0):
        tiles, chains = 8, 4
        w, r = sl // tiles, lat // chains
        if bv is not None:
            pb, inv = weights(bv, sv, mxv, 0, dst)
        top = None
        acc = [None] * chains
        for j in range(tiles):
            if bq is not None and j % 2 == 0:
                top = scores(bq, sq, j // 2, 2 * w, top)
            if bv is not None:
                c = cbuf.at[bv % SLOTS]
                for h in range(chains):
                    t = lax.dot_general(c[r * h:r * (h + 1), w * j:w * (j + 1)], pb[:, w * j:w * (j + 1)], NT,
                                        preferred_element_type=jnp.float32)
                    acc[h] = t if j == 0 else acc[h] + t
        if bv is not None:
            for h in range(chains):
                obuf[bv + 1, :, r * h:r * (h + 1)] = (acc[h].T * inv).astype(jnp.bfloat16)
        if bq is not None:
            mxq[...] = top

    lens.wait()
    lbuf[0] = jnp.zeros(lbuf.shape[1:], jnp.float32)
    forward_q(0)
    mate_copy(0, mate, mate).wait_recv()
    cache_copy(0).wait()
    cache_copy(1).wait()
    forward_q(1)
    wait_q(0)
    step(0, s_a, mx_a, None, None, None)
    step(1, s_b, mx_b, 0, s_a, mx_a)
    mate_copy(1, mate, mate).wait_recv()

    def body(k, _):
        @pl.when(k < pairs - 1)
        def _():
            forward_q(k + 1)

        wait_q(k)

        @pl.when(k < pairs - LEAD + 1)
        def _():
            q_copy(0, k + LEAD - 1, d, over).start()

        @pl.when(k < pairs - 2)
        def _():
            cache_copy(2 * k + 4).start()
            cache_copy(2 * k + 5).start()

        @pl.when(k == 1)
        def _():
            send_o(0)

        @pl.when(k > 1)
        def _():
            send_o(k - 1)

        cache_copy(2 * k).wait()
        cache_copy(2 * k + 1).wait()
        step(2 * k, s_a, mx_a, 2 * k - 1, s_b, mx_b)
        step(2 * k + 1, s_b, mx_b, 2 * k, s_a, mx_a)
        return 0

    lax.fori_loop(1, pairs, body, 0)

    def send_l(t):
        for i in (1, 2, 0):
            l_copy(t, i, d, peers[i]).start()

    send_o(pairs - 1)
    send_l(0)
    step(None, None, None, nb - 1, s_b, mx_b, 1)
    send_o(pairs)
    send_l(1)

    def shares(t):
        for i in (0, 1, 2):
            l_copy(t, i, peers[i], d).wait_recv()
        lses = [lbuf[t, rows(d), :]] + [lrecv[t, p] for p in peers]
        top = functools.reduce(jnp.maximum, lses)
        ws = [jnp.exp(x - top) for x in lses]
        norm = 1.0 / functools.reduce(jnp.add, ws)
        return [x * norm for x in ws]

    def merge(ws, b):
        lane = lax.broadcasted_iota(jnp.int32, ws[0].shape, 1)
        parts = [obuf[b + 1, rows(d), :]] + [orecv[p, b + 1] for p in peers]
        total = None
        for w, o in zip(ws, parts):
            col = jnp.sum(jnp.where(lane == b, w, 0.0), axis=1, keepdims=True)
            term = col * o.astype(jnp.float32)
            total = term if total is None else total + term
        out_ref[b] = total.astype(jnp.bfloat16)

    early = shares(0)
    wait_o(0)
    group = 6

    def merge_early(k, _):
        for r in range(group // 2):
            wait_o(group // 2 * k + r + 1)
        for r in range(group):
            merge(early, group * k + r)
        return 0

    lax.fori_loop(0, (nb - 2) // group, merge_early, 0)
    late = shares(1)
    wait_o(pairs)
    merge(late, nb - 2)
    merge(late, nb - 1)

    for t in (0, 1):
        for i in (0, 1, 2):
            l_copy(t, i, d, peers[i]).wait_send()
    for i in (0, 1):
        mate_copy(i, d, mate).wait_send()

    def drain(c, _):
        for i in (0, 1, 2):
            o_copy(i, c, d, peers[i]).wait_send()
        return 0

    lax.fori_loop(1, pairs, drain, 0)
    drain(0, 0)
    drain(pairs, 0)

    def drain_q(c, _):
        q_copy(0, c, d, over).wait_send()
        q_copy(1, c, over, mate).wait_send()
        return 0

    lax.fori_loop(0, pairs, drain_q, 0)


def solution(mesh):
    n = mesh.shape['dcp']

    def local(q, cache, lengths):
        b, own, wd = q.shape
        sl = cache.shape[1]
        lat = wd - ROPE
        heads = own * n
        vmem = pl.BlockSpec(memory_space=pltpu.VMEM)
        return pl.pallas_call(
            kernel,
            out_shape=jax.ShapeDtypeStruct((b, own, lat), jnp.bfloat16),
            in_specs=[
                pl.BlockSpec(memory_space=pltpu.HBM),
                pl.BlockSpec(memory_space=pltpu.HBM),
                pl.BlockSpec(memory_space=pltpu.HBM),
            ],
            out_specs=vmem,
            scratch_shapes=[
                pltpu.VMEM((SLOTS, wd, sl), jnp.bfloat16),
                pltpu.VMEM((b, heads, wd), jnp.bfloat16),
                pltpu.VMEM((heads, sl), jnp.float32),
                pltpu.VMEM((heads, sl), jnp.float32),
                pltpu.VMEM((heads, 128), jnp.float32),
                pltpu.VMEM((heads, 128), jnp.float32),
                pltpu.VMEM((b + 2, heads, lat), jnp.bfloat16),
                pltpu.VMEM((n, b + 2, own, lat), jnp.bfloat16),
                pltpu.VMEM((2, heads, 128), jnp.float32),
                pltpu.VMEM((2, n, own, 128), jnp.float32),
                pltpu.SMEM((b,), jnp.int32),
                pltpu.SemaphoreType.DMA,
                pltpu.SemaphoreType.DMA((SLOTS,)),
                pltpu.SemaphoreType.DMA,
                pltpu.SemaphoreType.DMA((2,)),
                pltpu.SemaphoreType.DMA((2,)),
                pltpu.SemaphoreType.DMA((2, b // 2)),
                pltpu.SemaphoreType.DMA((2, b // 2)),
                pltpu.SemaphoreType.DMA((3, b // 2 + 1)),
                pltpu.SemaphoreType.DMA((3, b // 2 + 1)),
                pltpu.SemaphoreType.DMA((2, 3)),
                pltpu.SemaphoreType.DMA((2, 3)),
            ],
            compiler_params=pltpu.CompilerParams(
                collective_id=0, has_side_effects=True, vmem_limit_bytes=40 * 2 ** 20
            ),
            name='mla_decode',
        )(pltpu.with_memory_space_constraint(lengths, pltpu.HBM), pltpu.with_memory_space_constraint(q, pltpu.HBM), jnp.swapaxes(cache, 1, 2))

    return jax.shard_map(local, mesh=mesh, in_specs=(P('dp', 'dcp', None), P('dp', 'dcp', None), P('dp')), out_specs=P('dp', 'dcp', None), check_vma=False)
```

```python
import functools

import jax
import jax.numpy as jnp
from jax import lax
from jax.experimental import pallas as pl
from jax.experimental.pallas import tpu as pltpu
from jax.sharding import PartitionSpec as P

ROPE = 64
SCALE = 192 ** -0.5
LOG2E = 1.4426950408889634
SLOTS = 8
NT = (((1,), (1,)), ((), ()))


def kernel(lens_ref, q_ref, cache_ref, out_ref, cbuf, qbuf, rbuf, rown, s_a, s_b, mx_a, mx_b, obuf, orecv, lbuf, lrecv, len_ref,
           n_sem, c_sem, q_sem, ms_sem, mr_sem, qs_sem, qr_sem, rs_sem, rr_sem, os_sem, or_sem, ls_sem, lr_sem):
    nb, heads, lat = qbuf.shape
    own = q_ref.shape[1]
    sl = cbuf.shape[2]
    pairs = nb // 2
    g = lax.axis_index('dp')
    d = lax.axis_index('dcp')
    mate = d + 1 - 2 * (d % 2)
    over = (d + 2) % 4
    far = mate + 2 - 4 * (mate // 2)
    peers = (mate, over, far)

    def rows(j):
        return pl.ds(pl.multiple_of(j * own, own), own)

    def cache_copy(b):
        slot = b % SLOTS
        return pltpu.make_async_copy(cache_ref.at[b], cbuf.at[slot], c_sem.at[slot])

    def remote(src, dst, ssem, rsem, dev):
        return pltpu.make_async_remote_copy(src_ref=src, dst_ref=dst, send_sem=ssem, recv_sem=rsem,
                                            device_id=(g, dev), device_id_type=pl.DeviceIdType.MESH)

    def seqs(m):
        if isinstance(m, int) and m < 2:
            return pl.ds(2 * m, 2)
        return pl.ds(4 * m - 4, 4)

    def q_copy(kind, m, src_dev, to):
        view = qbuf.at[seqs(m), rows(src_dev), :]
        return remote(view, view, qs_sem.at[kind, m], qr_sem.at[kind, m], to)

    def r_copy(kind, i, src_dev, to):
        view = rbuf.at[pl.ds(0, 2) if i == 0 else pl.ds(2, pairs - 2), rows(src_dev), :]
        return remote(view, view, rs_sem.at[kind, i], rr_sem.at[kind, i], to)

    def mate_copy(i, src_dev, to):
        if i == 2:
            view = rbuf.at[:, rows(src_dev), :]
        else:
            view = qbuf.at[pl.ds(0, 2) if i == 0 else pl.ds(2, nb - 2), rows(src_dev), :]
        return remote(view, view, ms_sem.at[i], mr_sem.at[i], to)

    last = nb // 4

    def o_copy(i, c, src_dev, dst_dev):
        if isinstance(c, int) and c in (0, last, last + 1):
            at = {0: pl.ds(1, 1), last: pl.ds(nb - 2, 2), last + 1: pl.ds(nb, 1)}[c]
        else:
            at = pl.ds(4 * c - 2, 4)
        return remote(obuf.at[at, rows(dst_dev), :], orecv.at[src_dev, at], os_sem.at[i, c], or_sem.at[i, c], dst_dev)

    def l_copy(t, i, src_dev, dst_dev):
        return remote(lbuf.at[t, rows(dst_dev), :], lrecv.at[t, src_dev], ls_sem.at[t, i], lr_sem.at[t, i], dst_dev)

    r_own = pltpu.make_async_copy(q_ref.at[:, :, pl.ds(lat, ROPE)], rown, q_sem.at[0])
    r_own.start()
    q_own = pltpu.make_async_copy(q_ref.at[:, :, pl.ds(0, lat)], qbuf.at[:, rows(d), :], q_sem.at[1])
    q_own.start()
    lens = pltpu.make_async_copy(lens_ref, len_ref, n_sem)
    lens.start()
    cache_copy(0).start()
    cache_copy(1).start()

    barrier = pltpu.get_barrier_semaphore()
    for p in peers:
        pl.semaphore_signal(barrier, inc=1, device_id=(g, p), device_id_type=pl.DeviceIdType.MESH)
    r_own.wait()
    for c in range(pairs):
        rbuf[c, rows(d), :] = jnp.concatenate([rown[2 * c], rown[2 * c + 1]], axis=1)
    lbuf[0] = jnp.zeros(lbuf.shape[1:], jnp.float32)
    pl.semaphore_wait(barrier, 3)

    q_own.wait()
    q_copy(0, 0, d, over).start()
    r_copy(0, 0, d, over).start()
    mate_copy(2, d, mate).start()
    mate_copy(0, d, mate).start()
    q_copy(0, 1, d, over).start()
    q_copy(0, 2, d, over).start()
    r_copy(0, 1, d, over).start()
    q_copy(0, 3, d, over).start()
    mate_copy(1, d, mate).start()
    for b in range(2, 6):
        cache_copy(b).start()

    def forward_q(m):
        q_copy(0, m, over, over).wait_recv()
        q_copy(1, m, over, mate).start()

    def forward_r(i):
        r_copy(0, i, over, over).wait_recv()
        r_copy(1, i, over, mate).start()

    def send_o(c):
        for i in (1, 2, 0):
            o_copy(i, c, d, peers[i]).start()

    def wait_o(c):
        for i in (0, 1, 2):
            o_copy(i, c, peers[i], d).wait_recv()

    def scores(k, odd, s_ref, j, w, top):
        b = 2 * k + odd
        n_valid = len_ref[b] - d * sl
        c = cbuf.at[b % SLOTS]
        q = jnp.concatenate([qbuf[b], rbuf[k, :, ROPE * odd:ROPE * (odd + 1)]], axis=1)
        s = jnp.dot(q, c[:, w * j:w * (j + 1)], preferred_element_type=jnp.float32)
        pos = lax.broadcasted_iota(jnp.int32, s.shape, 1) + w * j
        s = jnp.where(pos < n_valid, s, -jnp.inf)
        s_ref[:, w * j:w * (j + 1)] = s
        for k in range(w // 128):
            t = s[:, 128 * k:128 * (k + 1)]
            top = t if top is None else jnp.maximum(top, t)
        return top

    def weights(b, s_ref, mx_ref, src, dst):
        m = jnp.max(mx_ref[...], axis=1, keepdims=True)
        m0 = jnp.where(m == -jnp.inf, 0.0, m)
        p = jnp.exp2((s_ref[...] - m0) * (SCALE * LOG2E))
        l = jnp.sum(p, axis=1, keepdims=True)
        has = l > 0.0
        l1 = jnp.where(has, l, 1.0)
        lse = jnp.where(has, m0 * SCALE + jnp.log(l1), -jnp.inf)
        lane = lax.broadcasted_iota(jnp.int32, lbuf.shape[1:], 1)
        lbuf[dst] = jnp.where(lane == b, lse, lbuf[src])
        return p.astype(jnp.bfloat16), 1.0 / l1

    def step(kq, odd, sq, mxq, bv, sv, mxv, dst=0):
        tiles, chains = 8, 4
        w, r = sl // tiles, lat // chains
        if bv is not None:
            pb, inv = weights(bv, sv, mxv, 0, dst)
        top = None
        acc = [None] * chains
        for j in range(tiles):
            if kq is not None and j % 2 == 0:
                top = scores(kq, odd, sq, j // 2, 2 * w, top)
            if bv is not None:
                c = cbuf.at[bv % SLOTS]
                for h in range(chains):
                    t = lax.dot_general(c[r * h:r * (h + 1), w * j:w * (j + 1)], pb[:, w * j:w * (j + 1)], NT,
                                        preferred_element_type=jnp.float32)
                    acc[h] = t if j == 0 else acc[h] + t
        if bv is not None:
            for h in range(chains):
                obuf[bv + 1, :, r * h:r * (h + 1)] = (acc[h].T * inv).astype(jnp.bfloat16)
        if kq is not None:
            mxq[...] = top

    lens.wait()
    forward_q(0)
    forward_r(0)
    mate_copy(0, mate, mate).wait_recv()
    mate_copy(2, mate, mate).wait_recv()
    cache_copy(0).wait()
    cache_copy(1).wait()
    forward_q(1)
    q_copy(1, 0, far, mate).wait_recv()
    r_copy(1, 0, far, mate).wait_recv()
    step(0, 0, s_a, mx_a, None, None, None)
    step(0, 1, s_b, mx_b, 0, s_a, mx_a)
    mate_copy(1, mate, mate).wait_recv()

    def body(k, _):
        odd = k % 2 == 1

        @pl.when(k == 1)
        def _():
            forward_r(1)
            send_o(0)
            q_copy(1, 1, far, mate).wait_recv()

        @pl.when(jnp.logical_and(odd, k < pairs - 1))
        def _():
            forward_q((k + 1) // 2 + 1)

        @pl.when(jnp.logical_and(odd, k > 1))
        def _():
            send_o((k - 1) // 2)

        @pl.when(jnp.logical_and(odd, k < pairs - 6))
        def _():
            q_copy(0, (k - 1) // 2 + 4, d, over).start()

        @pl.when(k == 2)
        def _():
            r_copy(1, 1, far, mate).wait_recv()

        @pl.when(k % 2 == 0)
        def _():
            q_copy(1, k // 2 + 1, far, mate).wait_recv()

        @pl.when(k < pairs - 2)
        def _():
            cache_copy(2 * k + 4).start()
            cache_copy(2 * k + 5).start()

        cache_copy(2 * k).wait()
        cache_copy(2 * k + 1).wait()
        step(k, 0, s_a, mx_a, 2 * k - 1, s_b, mx_b)
        step(k, 1, s_b, mx_b, 2 * k, s_a, mx_a)
        return 0

    lax.fori_loop(1, pairs, body, 0)

    def send_l(t):
        for i in (1, 2, 0):
            l_copy(t, i, d, peers[i]).start()

    send_o(last)
    send_l(0)
    step(None, None, None, None, nb - 1, s_b, mx_b, 1)
    send_o(last + 1)
    send_l(1)

    def shares(t):
        for i in (0, 1, 2):
            l_copy(t, i, peers[i], d).wait_recv()
        lses = [lbuf[t, rows(d), :]] + [lrecv[t, p] for p in peers]
        top = functools.reduce(jnp.maximum, lses)
        ws = [jnp.exp(x - top) for x in lses]
        norm = 1.0 / functools.reduce(jnp.add, ws)
        return [x * norm for x in ws]

    def merge(ws, b):
        lane = lax.broadcasted_iota(jnp.int32, ws[0].shape, 1)
        parts = [obuf[b + 1, rows(d), :]] + [orecv[p, b + 1] for p in peers]
        total = None
        for w, o in zip(ws, parts):
            col = jnp.sum(jnp.where(lane == b, w, 0.0), axis=1, keepdims=True)
            term = col * o.astype(jnp.float32)
            total = term if total is None else total + term
        out_ref[b] = total.astype(jnp.bfloat16)

    early = shares(0)
    wait_o(0)
    merge(early, 0)

    def merge_early(m, _):
        wait_o(m)
        for r in range(4):
            merge(early, 4 * m - 3 + r)
        return 0

    lax.fori_loop(1, last, merge_early, 0)
    wait_o(last)
    merge(early, nb - 3)
    merge(early, nb - 2)
    late = shares(1)
    wait_o(last + 1)
    merge(late, nb - 1)

    for t in (0, 1):
        for i in (0, 1, 2):
            l_copy(t, i, d, peers[i]).wait_send()
    for i in (0, 1, 2):
        mate_copy(i, d, mate).wait_send()

    def drain(c, _):
        for i in (0, 1, 2):
            o_copy(i, c, d, peers[i]).wait_send()
        return 0

    lax.fori_loop(1, last, drain, 0)
    for c in (0, last, last + 1):
        drain(c, 0)

    def drain_q(m, _):
        q_copy(0, m, d, over).wait_send()
        q_copy(1, m, over, mate).wait_send()
        return 0

    lax.fori_loop(2, pairs // 2 + 1, drain_q, 0)
    for m in (0, 1):
        drain_q(m, 0)
        r_copy(0, m, d, over).wait_send()
        r_copy(1, m, over, mate).wait_send()


def solution(mesh):
    n = mesh.shape['dcp']

    def local(q, cache, lengths):
        b, own, wd = q.shape
        sl = cache.shape[1]
        lat = wd - ROPE
        heads = own * n
        vmem = pl.BlockSpec(memory_space=pltpu.VMEM)
        dma = pltpu.SemaphoreType.DMA
        return pl.pallas_call(
            kernel,
            out_shape=jax.ShapeDtypeStruct((b, own, lat), jnp.bfloat16),
            in_specs=[
                pl.BlockSpec(memory_space=pltpu.HBM),
                pl.BlockSpec(memory_space=pltpu.HBM),
                pl.BlockSpec(memory_space=pltpu.HBM),
            ],
            out_specs=vmem,
            scratch_shapes=[
                pltpu.VMEM((SLOTS, wd, sl), jnp.bfloat16),
                pltpu.VMEM((b, heads, lat), jnp.bfloat16),
                pltpu.VMEM((b // 2, heads, 2 * ROPE), jnp.bfloat16),
                pltpu.VMEM((b, own, ROPE), jnp.bfloat16),
                pltpu.VMEM((heads, sl), jnp.float32),
                pltpu.VMEM((heads, sl), jnp.float32),
                pltpu.VMEM((heads, 128), jnp.float32),
                pltpu.VMEM((heads, 128), jnp.float32),
                pltpu.VMEM((b + 2, heads, lat), jnp.bfloat16),
                pltpu.VMEM((n, b + 2, own, lat), jnp.bfloat16),
                pltpu.VMEM((2, heads, 128), jnp.float32),
                pltpu.VMEM((2, n, own, 128), jnp.float32),
                pltpu.SMEM((b,), jnp.int32),
                dma,
                dma((SLOTS,)),
                dma((2,)),
                dma((3,)),
                dma((3,)),
                dma((2, b // 4 + 1)),
                dma((2, b // 4 + 1)),
                dma((2, 2)),
                dma((2, 2)),
                dma((3, b // 4 + 2)),
                dma((3, b // 4 + 2)),
                dma((2, 3)),
                dma((2, 3)),
            ],
            compiler_params=pltpu.CompilerParams(
                collective_id=0, has_side_effects=True, vmem_limit_bytes=40 * 2 ** 20
            ),
            name='mla_decode',
        )(pltpu.with_memory_space_constraint(lengths, pltpu.HBM), pltpu.with_memory_space_constraint(q, pltpu.HBM), jnp.swapaxes(cache, 1, 2))

    return jax.shard_map(local, mesh=mesh, in_specs=(P('dp', 'dcp', None), P('dp', 'dcp', None), P('dp')), out_specs=P('dp', 'dcp', None), check_vma=False)
```

```python
import functools

import jax
import jax.numpy as jnp
from jax import lax
from jax.experimental import pallas as pl
from jax.experimental.pallas import tpu as pltpu
from jax.sharding import PartitionSpec as P

ROPE = 64
SCALE = 192 ** -0.5
LOG2E = 1.4426950408889634
SLOTS = 8
LEAD = 5
NT = (((1,), (1,)), ((), ()))


def kernel(lens_ref, q_ref, cache_ref, out_ref, cbuf, qbuf, s_a, s_b, mx_a, mx_b, obuf, orecv, lbuf, lrecv, len_ref,
           n_sem, c_sem, q_sem, ms_sem, mr_sem, qs_sem, qr_sem, os_sem, or_sem, ls_sem, lr_sem):
    nb, heads, wd = qbuf.shape
    own = q_ref.shape[1]
    lat = wd - ROPE
    sl = cbuf.shape[2]
    pairs = nb // 2
    g = lax.axis_index('dp')
    d = lax.axis_index('dcp')
    mate = d + 1 - 2 * (d % 2)
    over = (d + 2) % 4
    far = mate + 2 - 4 * (mate // 2)
    peers = (mate, over, far)

    def rows(j):
        return pl.ds(pl.multiple_of(j * own, own), own)

    def cache_copy(b):
        slot = b % SLOTS
        return pltpu.make_async_copy(cache_ref.at[b], cbuf.at[slot], c_sem.at[slot])

    def remote(src, dst, ssem, rsem, dev):
        return pltpu.make_async_remote_copy(src_ref=src, dst_ref=dst, send_sem=ssem, recv_sem=rsem,
                                            device_id=(g, dev), device_id_type=pl.DeviceIdType.MESH)

    def mate_copy(i, src_dev, to):
        view = qbuf.at[pl.ds(0, 2) if i == 0 else pl.ds(2, nb - 2), rows(src_dev), :]
        return remote(view, view, ms_sem.at[i], mr_sem.at[i], to)

    def q_copy(kind, c, src_dev, to):
        view = qbuf.at[pl.ds(2 * c, 2), rows(src_dev), :]
        return remote(view, view, qs_sem.at[kind, c], qr_sem.at[kind, c], to)

    def o_copy(i, c, src_dev, dst_dev):
        if isinstance(c, int) and (c == 0 or c >= pairs - 1):
            at = pl.ds(1 if c == 0 else c + pairs - 1, 1)
        else:
            at = pl.ds(2 * c, 2)
        return remote(obuf.at[at, rows(dst_dev), :], orecv.at[src_dev, at], os_sem.at[i, c], or_sem.at[i, c], dst_dev)

    def l_copy(t, i, src_dev, dst_dev):
        return remote(lbuf.at[t, rows(dst_dev), :], lrecv.at[t, src_dev], ls_sem.at[t, i], lr_sem.at[t, i], dst_dev)

    q_own = pltpu.make_async_copy(q_ref, qbuf.at[:, rows(d), :], q_sem)
    q_own.start()
    lens = pltpu.make_async_copy(lens_ref, len_ref, n_sem)
    lens.start()

    barrier = pltpu.get_barrier_semaphore()
    for p in peers:
        pl.semaphore_signal(barrier, inc=1, device_id=(g, p), device_id_type=pl.DeviceIdType.MESH)
    pl.semaphore_wait(barrier, 3)

    q_own.wait()
    q_copy(0, 0, d, over).start()
    mate_copy(0, d, mate).start()
    cache_copy(0).start()
    for c in range(1, LEAD):
        q_copy(0, c, d, over).start()
    cache_copy(1).start()

    def forward_q(c):
        q_copy(0, c, over, over).wait_recv()
        q_copy(1, c, over, mate).start()

    def wait_q(c):
        q_copy(1, c, far, mate).wait_recv()

    def send_o(c):
        for i in (1, 2, 0):
            o_copy(i, c, d, peers[i]).start()

    def wait_o(c):
        for i in (0, 1, 2):
            o_copy(i, c, peers[i], d).wait_recv()

    def scores(b, s_ref, j, w, top):
        n_valid = len_ref[b] - d * sl
        c = cbuf.at[b % SLOTS]
        s = jnp.dot(qbuf[b], c[:, w * j:w * (j + 1)], preferred_element_type=jnp.float32)
        pos = lax.broadcasted_iota(jnp.int32, s.shape, 1) + w * j
        s = jnp.where(pos < n_valid, s, -jnp.inf)
        s_ref[:, w * j:w * (j + 1)] = s
        for k in range(w // 128):
            t = s[:, 128 * k:128 * (k + 1)]
            top = t if top is None else jnp.maximum(top, t)
        return top

    def weights(b, s_ref, mx_ref, src, dst):
        m = jnp.max(mx_ref[...], axis=1, keepdims=True)
        m0 = jnp.where(m == -jnp.inf, 0.0, m)
        p = jnp.exp2((s_ref[...] - m0) * (SCALE * LOG2E))
        l = jnp.sum(p, axis=1, keepdims=True)
        has = l > 0.0
        l1 = jnp.where(has, l, 1.0)
        lse = jnp.where(has, m0 * SCALE + jnp.log(l1), -jnp.inf)
        lane = lax.broadcasted_iota(jnp.int32, lbuf.shape[1:], 1)
        lbuf[dst] = jnp.where(lane == b, lse, lbuf[src])
        return p.astype(jnp.bfloat16), 1.0 / l1

    def step(bq, sq, mxq, bv, sv, mxv, dst=0, at=(0, 2, 4, 6)):
        tiles, chains = 8, 4
        w, r = sl // tiles, lat // chains
        if bv is not None:
            pb, inv = weights(bv, sv, mxv, 0, dst)
        top = None
        acc = [None] * chains
        for j in range(tiles + 1):
            if bq is not None and j in at:
                top = scores(bq, sq, at.index(j), 2 * w, top)
            if bv is not None and j < tiles:
                c = cbuf.at[bv % SLOTS]
                for h in range(chains):
                    t = lax.dot_general(c[r * h:r * (h + 1), w * j:w * (j + 1)], pb[:, w * j:w * (j + 1)], NT,
                                        preferred_element_type=jnp.float32)
                    acc[h] = t if j == 0 else acc[h] + t
        if bv is not None:
            for h in range(chains):
                obuf[bv + 1, :, r * h:r * (h + 1)] = (acc[h].T * inv).astype(jnp.bfloat16)
        if bq is not None:
            mxq[...] = top

    lbuf[0] = jnp.zeros(lbuf.shape[1:], jnp.float32)
    lens.wait()
    forward_q(0)
    mate_copy(1, d, mate).start()
    cache_copy(2).start()
    cache_copy(3).start()
    mate_copy(0, mate, mate).wait_recv()
    cache_copy(0).wait()
    cache_copy(1).wait()
    forward_q(1)
    cache_copy(4).start()
    cache_copy(5).start()
    wait_q(0)
    step(0, s_a, mx_a, None, None, None)
    step(1, s_b, mx_b, 0, s_a, mx_a)
    mate_copy(1, mate, mate).wait_recv()

    def enter(k):
        if not isinstance(k, int):
            @pl.when(k < pairs - 1)
            def _():
                forward_q(k + 1)

        wait_q(k)
        if not isinstance(k, int):
            @pl.when(k < pairs - LEAD + 1)
            def _():
                q_copy(0, k + LEAD - 1, d, over).start()

            @pl.when(k < pairs - 2)
            def _():
                cache_copy(2 * k + 4).start()
                cache_copy(2 * k + 5).start()

            @pl.when(k == 1)
            def _():
                send_o(0)

            @pl.when(k > 1)
            def _():
                send_o(k - 1)
        else:
            send_o(k - 1)

        cache_copy(2 * k).wait()
        cache_copy(2 * k + 1).wait()

    def first(k):
        step(2 * k, s_a, mx_a, 2 * k - 1, s_b, mx_b)

    def second(k):
        step(2 * k + 1, s_b, mx_b, 2 * k, s_a, mx_a, at=(0, 2, 4, 8))

    def body(k, _):
        enter(k)
        first(k)
        second(k)
        return 0

    lax.fori_loop(1, pairs - 1, body, 0)

    def send_l(t):
        for i in (1, 2, 0):
            l_copy(t, i, d, peers[i]).start()

    enter(pairs - 1)
    first(pairs - 1)
    send_o(pairs - 1)
    second(pairs - 1)
    send_o(pairs)
    send_l(0)
    step(None, None, None, nb - 1, s_b, mx_b, 1)
    send_o(pairs + 1)
    send_l(1)

    def shares(t):
        for i in (0, 1, 2):
            l_copy(t, i, peers[i], d).wait_recv()
        lses = [lbuf[t, rows(d), :]] + [lrecv[t, p] for p in peers]
        top = functools.reduce(jnp.maximum, lses)
        ws = [jnp.exp(x - top) for x in lses]
        norm = 1.0 / functools.reduce(jnp.add, ws)
        return [x * norm for x in ws]

    def merge(ws, b):
        lane = lax.broadcasted_iota(jnp.int32, ws[0].shape, 1)
        parts = [obuf[b + 1, rows(d), :]] + [orecv[p, b + 1] for p in peers]
        total = None
        for w, o in zip(ws, parts):
            col = jnp.sum(jnp.where(lane == b, w, 0.0), axis=1, keepdims=True)
            term = col * o.astype(jnp.float32)
            total = term if total is None else total + term
        out_ref[b] = total.astype(jnp.bfloat16)

    early = shares(0)
    wait_o(0)
    group = 6

    def merge_early(k, _):
        for r in range(group // 2):
            wait_o(group // 2 * k + r + 1)
        for r in range(group):
            merge(early, group * k + r)
        return 0

    whole = (nb - 3) // group
    lax.fori_loop(0, whole, merge_early, 0)
    for c in range(group // 2 * whole + 1, pairs - 1):
        wait_o(c)
    for b in range(group * whole, nb - 3):
        merge(early, b)
    for b in (nb - 3, nb - 2):
        wait_o(b - pairs + 2)
        merge(early, b)
    late = shares(1)
    wait_o(pairs + 1)
    merge(late, nb - 1)

    for t in (0, 1):
        for i in (0, 1, 2):
            l_copy(t, i, d, peers[i]).wait_send()
    for i in (0, 1):
        mate_copy(i, d, mate).wait_send()

    def drain(c, _):
        for i in (0, 1, 2):
            o_copy(i, c, d, peers[i]).wait_send()
        return 0

    lax.fori_loop(1, pairs - 1, drain, 0)
    for c in (0, pairs - 1, pairs, pairs + 1):
        drain(c, 0)

    def drain_q(c, _):
        q_copy(0, c, d, over).wait_send()
        q_copy(1, c, over, mate).wait_send()
        return 0

    lax.fori_loop(0, pairs, drain_q, 0)


def solution(mesh):
    n = mesh.shape['dcp']

    def local(q, cache, lengths):
        b, own, wd = q.shape
        sl = cache.shape[1]
        lat = wd - ROPE
        heads = own * n
        vmem = pl.BlockSpec(memory_space=pltpu.VMEM)
        return pl.pallas_call(
            kernel,
            out_shape=jax.ShapeDtypeStruct((b, own, lat), jnp.bfloat16),
            in_specs=[
                pl.BlockSpec(memory_space=pltpu.HBM),
                pl.BlockSpec(memory_space=pltpu.HBM),
                pl.BlockSpec(memory_space=pltpu.HBM),
            ],
            out_specs=vmem,
            scratch_shapes=[
                pltpu.VMEM((SLOTS, wd, sl), jnp.bfloat16),
                pltpu.VMEM((b, heads, wd), jnp.bfloat16),
                pltpu.VMEM((heads, sl), jnp.float32),
                pltpu.VMEM((heads, sl), jnp.float32),
                pltpu.VMEM((heads, 128), jnp.float32),
                pltpu.VMEM((heads, 128), jnp.float32),
                pltpu.VMEM((b + 2, heads, lat), jnp.bfloat16),
                pltpu.VMEM((n, b + 2, own, lat), jnp.bfloat16),
                pltpu.VMEM((2, heads, 128), jnp.float32),
                pltpu.VMEM((2, n, own, 128), jnp.float32),
                pltpu.SMEM((b,), jnp.int32),
                pltpu.SemaphoreType.DMA,
                pltpu.SemaphoreType.DMA((SLOTS,)),
                pltpu.SemaphoreType.DMA,
                pltpu.SemaphoreType.DMA((2,)),
                pltpu.SemaphoreType.DMA((2,)),
                pltpu.SemaphoreType.DMA((2, b // 2)),
                pltpu.SemaphoreType.DMA((2, b // 2)),
                pltpu.SemaphoreType.DMA((3, b // 2 + 2)),
                pltpu.SemaphoreType.DMA((3, b // 2 + 2)),
                pltpu.SemaphoreType.DMA((2, 3)),
                pltpu.SemaphoreType.DMA((2, 3)),
            ],
            compiler_params=pltpu.CompilerParams(
                collective_id=0, has_side_effects=True, vmem_limit_bytes=40 * 2 ** 20
            ),
            name='mla_decode',
        )(pltpu.with_memory_space_constraint(lengths, pltpu.HBM), pltpu.with_memory_space_constraint(q, pltpu.HBM), jnp.swapaxes(cache, 1, 2))

    return jax.shard_map(local, mesh=mesh, in_specs=(P('dp', 'dcp', None), P('dp', 'dcp', None), P('dp')), out_specs=P('dp', 'dcp', None), check_vma=False)
```

```python
import functools

import jax
import jax.numpy as jnp
from jax import lax
from jax.experimental import pallas as pl
from jax.experimental.pallas import tpu as pltpu
from jax.sharding import PartitionSpec as P

ROPE = 64
SCALE = 192 ** -0.5
LOG2E = 1.4426950408889634
SLOTS = 12
LEAD = 7
NT = (((1,), (1,)), ((), ()))


def kernel(lens_ref, q_ref, cache_ref, out_ref, cbuf, qbuf, s_a, s_b, mx_a, mx_b, obuf, orecv, lbuf, lrecv, len_ref,
           n_sem, c_sem, q_sem, ms_sem, mr_sem, qs_sem, qr_sem, os_sem, or_sem, ls_sem, lr_sem):
    nb, heads, wd = qbuf.shape
    own = q_ref.shape[1]
    lat = wd - ROPE
    sl = cbuf.shape[2]
    pairs = nb // 2
    g = lax.axis_index('dp')
    d = lax.axis_index('dcp')
    mate = d + 1 - 2 * (d % 2)
    over = (d + 2) % 4
    far = mate + 2 - 4 * (mate // 2)
    peers = (mate, over, far)

    def rows(j):
        return pl.ds(pl.multiple_of(j * own, own), own)

    def cache_copy(b):
        slot = b % SLOTS
        return pltpu.make_async_copy(cache_ref.at[b], cbuf.at[slot], c_sem.at[slot])

    def remote(src, dst, ssem, rsem, dev):
        return pltpu.make_async_remote_copy(src_ref=src, dst_ref=dst, send_sem=ssem, recv_sem=rsem,
                                            device_id=(g, dev), device_id_type=pl.DeviceIdType.MESH)

    def mate_copy(i, src_dev, to):
        view = qbuf.at[pl.ds(0, 2) if i == 0 else pl.ds(2, nb - 2), rows(src_dev), :]
        return remote(view, view, ms_sem.at[i], mr_sem.at[i], to)

    def q_copy(kind, c, src_dev, to):
        view = qbuf.at[pl.ds(2 * c, 2), rows(src_dev), :]
        return remote(view, view, qs_sem.at[kind, c], qr_sem.at[kind, c], to)

    quads = nb // 4

    def o_copy(i, c, src_dev, dst_dev):
        if isinstance(c, int) and (c == 0 or c >= quads):
            at = pl.ds(1 if c == 0 else c + nb - 2 - quads, 1)
        else:
            at = pl.ds(4 * c - 2, 4)
        return remote(obuf.at[at, rows(dst_dev), :], orecv.at[src_dev, at], os_sem.at[i, c], or_sem.at[i, c], dst_dev)

    def l_copy(t, i, src_dev, dst_dev):
        return remote(lbuf.at[t, rows(dst_dev), :], lrecv.at[t, src_dev], ls_sem.at[t, i], lr_sem.at[t, i], dst_dev)

    q_own = pltpu.make_async_copy(q_ref, qbuf.at[:, rows(d), :], q_sem)
    q_own.start()
    lens = pltpu.make_async_copy(lens_ref, len_ref, n_sem)
    lens.start()

    barrier = pltpu.get_barrier_semaphore()
    for p in peers:
        pl.semaphore_signal(barrier, inc=1, device_id=(g, p), device_id_type=pl.DeviceIdType.MESH)
    pl.semaphore_wait(barrier, 3)

    q_own.wait()
    q_copy(0, 0, d, over).start()
    mate_copy(0, d, mate).start()
    cache_copy(0).start()
    for c in range(1, LEAD):
        q_copy(0, c, d, over).start()
    cache_copy(1).start()

    def forward_q(c):
        q_copy(0, c, over, over).wait_recv()
        q_copy(1, c, over, mate).start()

    def wait_q(c):
        q_copy(1, c, far, mate).wait_recv()

    def send_o(c):
        for i in (1, 2, 0):
            o_copy(i, c, d, peers[i]).start()

    def wait_o(c):
        for i in (0, 1, 2):
            o_copy(i, c, peers[i], d).wait_recv()

    def scores(b, s_ref, j, w, top):
        n_valid = len_ref[b] - d * sl
        c = cbuf.at[b % SLOTS]
        s = jnp.dot(qbuf[b], c[:, w * j:w * (j + 1)], preferred_element_type=jnp.float32)
        pos = lax.broadcasted_iota(jnp.int32, s.shape, 1) + w * j
        s = jnp.where(pos < n_valid, s, -jnp.inf)
        s_ref[:, w * j:w * (j + 1)] = s
        for k in range(w // 128):
            t = s[:, 128 * k:128 * (k + 1)]
            top = t if top is None else jnp.maximum(top, t)
        return top

    def weights(b, s_ref, mx_ref, src, dst):
        m = jnp.max(mx_ref[...], axis=1, keepdims=True)
        m0 = jnp.where(m == -jnp.inf, 0.0, m)
        p = jnp.exp2((s_ref[...] - m0) * (SCALE * LOG2E))
        l = jnp.sum(p, axis=1, keepdims=True)
        has = l > 0.0
        l1 = jnp.where(has, l, 1.0)
        lse = jnp.where(has, m0 * SCALE + jnp.log(l1), -jnp.inf)
        lane = lax.broadcasted_iota(jnp.int32, lbuf.shape[1:], 1)
        lbuf[dst] = jnp.where(lane == b, lse, lbuf[src])
        return p.astype(jnp.bfloat16), 1.0 / l1

    def step(bq, sq, mxq, bv, sv, mxv, dst=0, at=(0, 2, 4, 6)):
        tiles, chains = 8, 4
        w, r = sl // tiles, lat // chains
        if bv is not None:
            pb, inv = weights(bv, sv, mxv, 0, dst)
        top = None
        acc = [None] * chains
        for j in range(tiles + 1):
            if bq is not None and j in at:
                top = scores(bq, sq, at.index(j), 2 * w, top)
            if bv is not None and j < tiles:
                c = cbuf.at[bv % SLOTS]
                for h in range(chains):
                    t = lax.dot_general(c[r * h:r * (h + 1), w * j:w * (j + 1)], pb[:, w * j:w * (j + 1)], NT,
                                        preferred_element_type=jnp.float32)
                    acc[h] = t if j == 0 else acc[h] + t
        if bv is not None:
            for h in range(chains):
                obuf[bv + 1, :, r * h:r * (h + 1)] = (acc[h].T * inv).astype(jnp.bfloat16)
        if bq is not None:
            mxq[...] = top

    lbuf[0] = jnp.zeros(lbuf.shape[1:], jnp.float32)
    lens.wait()
    forward_q(0)
    mate_copy(1, d, mate).start()
    cache_copy(2).start()
    cache_copy(3).start()
    mate_copy(0, mate, mate).wait_recv()
    cache_copy(0).wait()
    cache_copy(1).wait()
    wait_q(0)
    step(0, s_a, mx_a, None, None, None)
    forward_q(1)
    forward_q(2)
    cache_copy(4).start()
    cache_copy(5).start()
    step(1, s_b, mx_b, 0, s_a, mx_a)
    mate_copy(1, mate, mate).wait_recv()

    def enter(m):
        for c in (2 * m + 3, 2 * m + 4):
            @pl.when(c < pairs)
            def _():
                forward_q(c)

        for c in (2 * m + LEAD, 2 * m + LEAD + 1):
            @pl.when(c < pairs)
            def _():
                q_copy(0, c, d, over).start()

        @pl.when(m == 0)
        def _():
            send_o(0)

        @pl.when(m > 0)
        def _():
            send_o(m)

        for b in range(6, 10):
            @pl.when(4 * m + b < nb)
            def _():
                cache_copy(4 * m + b).start()

        for c in (1, 2):
            wait_q(2 * m + c)
        for b in range(2, 6):
            cache_copy(4 * m + b).wait()

    def first(k, at=(0,2,4,6)):
        step(2 * k, s_a, mx_a, 2 * k - 1, s_b, mx_b, at=at)

    def second(k, at=(0,2,4,8)):
        step(2 * k + 1, s_b, mx_b, 2 * k, s_a, mx_a, at=at)

    def body(m, _):
        enter(m)
        first(2 * m + 1)
        second(2 * m + 1, (0,2,4,6))
        first(2 * m + 2)
        second(2 * m + 2)
        return 0

    lax.fori_loop(0, quads - 1, body, 0)

    def send_l(t):
        for i in (1, 2, 0):
            l_copy(t, i, d, peers[i]).start()

    send_o(quads - 1)
    wait_q(pairs - 1)
    cache_copy(nb - 2).wait()
    cache_copy(nb - 1).wait()
    first(pairs - 1)
    send_o(quads)
    second(pairs - 1)
    send_o(quads + 1)
    send_l(0)
    step(None, None, None, nb - 1, s_b, mx_b, 1)
    send_o(quads + 2)
    send_l(1)

    def shares(t):
        for i in (0, 1, 2):
            l_copy(t, i, peers[i], d).wait_recv()
        lses = [lbuf[t, rows(d), :]] + [lrecv[t, p] for p in peers]
        top = functools.reduce(jnp.maximum, lses)
        ws = [jnp.exp(x - top) for x in lses]
        norm = 1.0 / functools.reduce(jnp.add, ws)
        return [x * norm for x in ws]

    def merge(ws, b):
        lane = lax.broadcasted_iota(jnp.int32, ws[0].shape, 1)
        parts = [obuf[b + 1, rows(d), :]] + [orecv[p, b + 1] for p in peers]
        total = None
        for w, o in zip(ws, parts):
            col = jnp.sum(jnp.where(lane == b, w, 0.0), axis=1, keepdims=True)
            term = col * o.astype(jnp.float32)
            total = term if total is None else total + term
        out_ref[b] = total.astype(jnp.bfloat16)

    early = shares(0)
    wait_o(0)
    merge(early, 0)

    def merge_early(t, _):
        for c in (2 * t + 1, 2 * t + 2):
            wait_o(c)
        for r in range(8):
            merge(early, 8 * t + 1 + r)
        return 0

    lax.fori_loop(0, (quads - 1) // 2, merge_early, 0)
    wait_o(quads - 1)
    for b in range(nb - 7, nb - 3):
        merge(early, b)
    for b in (nb - 3, nb - 2):
        wait_o(b - nb + 3 + quads)
        merge(early, b)
    late = shares(1)
    wait_o(quads + 2)
    merge(late, nb - 1)

    for t in (0, 1):
        for i in (0, 1, 2):
            l_copy(t, i, d, peers[i]).wait_send()
    for i in (0, 1):
        mate_copy(i, d, mate).wait_send()

    def drain(c, _):
        for i in (0, 1, 2):
            o_copy(i, c, d, peers[i]).wait_send()
        return 0

    lax.fori_loop(1, quads, drain, 0)
    for c in (0, quads, quads + 1, quads + 2):
        drain(c, 0)

    def drain_q(c, _):
        q_copy(0, c, d, over).wait_send()
        q_copy(1, c, over, mate).wait_send()
        return 0

    lax.fori_loop(0, pairs, drain_q, 0)


def solution(mesh):
    n = mesh.shape['dcp']

    def local(q, cache, lengths):
        b, own, wd = q.shape
        sl = cache.shape[1]
        lat = wd - ROPE
        heads = own * n
        vmem = pl.BlockSpec(memory_space=pltpu.VMEM)
        return pl.pallas_call(
            kernel,
            out_shape=jax.ShapeDtypeStruct((b, own, lat), jnp.bfloat16),
            in_specs=[
                pl.BlockSpec(memory_space=pltpu.HBM),
                pl.BlockSpec(memory_space=pltpu.HBM),
                pl.BlockSpec(memory_space=pltpu.HBM),
            ],
            out_specs=vmem,
            scratch_shapes=[
                pltpu.VMEM((SLOTS, wd, sl), jnp.bfloat16),
                pltpu.VMEM((b, heads, wd), jnp.bfloat16),
                pltpu.VMEM((heads, sl), jnp.float32),
                pltpu.VMEM((heads, sl), jnp.float32),
                pltpu.VMEM((heads, 128), jnp.float32),
                pltpu.VMEM((heads, 128), jnp.float32),
                pltpu.VMEM((b + 2, heads, lat), jnp.bfloat16),
                pltpu.VMEM((n, b + 2, own, lat), jnp.bfloat16),
                pltpu.VMEM((2, heads, 128), jnp.float32),
                pltpu.VMEM((2, n, own, 128), jnp.float32),
                pltpu.SMEM((b,), jnp.int32),
                pltpu.SemaphoreType.DMA,
                pltpu.SemaphoreType.DMA((SLOTS,)),
                pltpu.SemaphoreType.DMA,
                pltpu.SemaphoreType.DMA((2,)),
                pltpu.SemaphoreType.DMA((2,)),
                pltpu.SemaphoreType.DMA((2, b // 2)),
                pltpu.SemaphoreType.DMA((2, b // 2)),
                pltpu.SemaphoreType.DMA((3, b // 4 + 3)),
                pltpu.SemaphoreType.DMA((3, b // 4 + 3)),
                pltpu.SemaphoreType.DMA((2, 3)),
                pltpu.SemaphoreType.DMA((2, 3)),
            ],
            compiler_params=pltpu.CompilerParams(
                collective_id=0, has_side_effects=True, vmem_limit_bytes=46 * 2 ** 20
            ),
            name='mla_decode',
        )(pltpu.with_memory_space_constraint(lengths, pltpu.HBM), pltpu.with_memory_space_constraint(q, pltpu.HBM), jnp.swapaxes(cache, 1, 2))

    return jax.shard_map(local, mesh=mesh, in_specs=(P('dp', 'dcp', None), P('dp', 'dcp', None), P('dp')), out_specs=P('dp', 'dcp', None), check_vma=False)
```

```python
import functools

import jax
import jax.numpy as jnp
from jax import lax
from jax.experimental import pallas as pl
from jax.experimental.pallas import tpu as pltpu
from jax.sharding import PartitionSpec as P

ROPE = 64
SCALE = 192 ** -0.5
LOG2E = 1.4426950408889634
SLOTS = 8
LEAD = 5
NT = (((1,), (1,)), ((), ()))


def kernel(lens_ref, q_ref, cache_ref, out_ref, cbuf, qbuf, s_a, s_b, mx_a, mx_b, obuf, orecv, lbuf, lrecv, len_ref,
           n_sem, c_sem, q_sem, ms_sem, mr_sem, qs_sem, qr_sem, os_sem, or_sem, ls_sem, lr_sem):
    nb, heads, wd = qbuf.shape
    own = q_ref.shape[1]
    lat = wd - ROPE
    sl = cbuf.shape[2]
    pairs = nb // 2
    g = lax.axis_index('dp')
    d = lax.axis_index('dcp')
    mate = d + 1 - 2 * (d % 2)
    over = (d + 2) % 4
    far = mate + 2 - 4 * (mate // 2)
    peers = (mate, over, far)

    def rows(j):
        return pl.ds(pl.multiple_of(j * own, own), own)

    def cache_copy(b):
        slot = b % SLOTS
        return pltpu.make_async_copy(cache_ref.at[b], cbuf.at[slot], c_sem.at[slot])

    def remote(src, dst, ssem, rsem, dev):
        return pltpu.make_async_remote_copy(src_ref=src, dst_ref=dst, send_sem=ssem, recv_sem=rsem,
                                            device_id=(g, dev), device_id_type=pl.DeviceIdType.MESH)

    def mate_copy(i, src_dev, to):
        view = qbuf.at[pl.ds(0, 2) if i == 0 else pl.ds(2, nb - 2), rows(src_dev), :]
        return remote(view, view, ms_sem.at[i], mr_sem.at[i], to)

    def q_copy(kind, c, src_dev, to):
        view = qbuf.at[pl.ds(2 * c, 2), rows(src_dev), :]
        return remote(view, view, qs_sem.at[kind, c], qr_sem.at[kind, c], to)

    def o_copy(i, c, src_dev, dst_dev):
        if isinstance(c, int) and (c == 0 or c >= pairs - 1):
            at = pl.ds(1 if c == 0 else c + pairs - 1, 1)
        else:
            at = pl.ds(2 * c, 2)
        return remote(obuf.at[at, rows(dst_dev), :], orecv.at[src_dev, at], os_sem.at[i, c], or_sem.at[i, c], dst_dev)

    def l_copy(i, src_dev, dst_dev):
        return remote(lbuf.at[rows(dst_dev), :], lrecv.at[src_dev], ls_sem.at[i], lr_sem.at[i], dst_dev)

    q_own = pltpu.make_async_copy(q_ref, qbuf.at[:, rows(d), :], q_sem)
    q_own.start()
    lens = pltpu.make_async_copy(lens_ref, len_ref, n_sem)
    lens.start()

    barrier = pltpu.get_barrier_semaphore()
    for p in peers:
        pl.semaphore_signal(barrier, inc=1, device_id=(g, p), device_id_type=pl.DeviceIdType.MESH)
    pl.semaphore_wait(barrier, 3)

    q_own.wait()
    q_copy(0, 0, d, over).start()
    mate_copy(0, d, mate).start()
    cache_copy(0).start()
    for c in range(1, LEAD):
        q_copy(0, c, d, over).start()
    cache_copy(1).start()

    def forward_q(c):
        q_copy(0, c, over, over).wait_recv()
        q_copy(1, c, over, mate).start()

    def wait_q(c):
        q_copy(1, c, far, mate).wait_recv()

    def send_o(c):
        for i in (1, 2, 0):
            o_copy(i, c, d, peers[i]).start()

    def wait_o(c):
        for i in (0, 1, 2):
            o_copy(i, c, peers[i], d).wait_recv()

    def scores(b, s_ref, j, w, top):
        n_valid = len_ref[b] - d * sl
        c = cbuf.at[b % SLOTS]
        s = jnp.dot(qbuf[b], c[:, w * j:w * (j + 1)], preferred_element_type=jnp.float32)
        pos = lax.broadcasted_iota(jnp.int32, s.shape, 1) + w * j
        s = jnp.where(pos < n_valid, s, -jnp.inf)
        s_ref[:, w * j:w * (j + 1)] = s
        for k in range(w // 128):
            t = s[:, 128 * k:128 * (k + 1)]
            top = t if top is None else jnp.maximum(top, t)
        return top

    def weights(b, s_ref, mx_ref):
        m = jnp.max(mx_ref[...], axis=1, keepdims=True)
        m0 = jnp.where(m == -jnp.inf, 0.0, m)
        p = jnp.exp2((s_ref[...] - m0) * (SCALE * LOG2E))
        l = jnp.sum(p, axis=1, keepdims=True)
        has = l > 0.0
        l1 = jnp.where(has, l, 1.0)
        lse = jnp.where(has, m0 * SCALE + jnp.log(l1), -jnp.inf)
        lane = lax.broadcasted_iota(jnp.int32, lbuf.shape, 1)
        lbuf[...] = jnp.where(lane == b, lse, lbuf[...])
        return p.astype(jnp.bfloat16), 1.0 / l1

    def step(bq, sq, mxq, bv, sv, mxv, at=(0, 2, 4, 6), known=None):
        tiles, chains = 8, 4
        w, r = sl // tiles, lat // chains
        if bv is not None:
            pb, inv = weights(bv, sv, mxv)
            if known is not None:
                known()
        top = None
        acc = [None] * chains
        for j in range(tiles + 1):
            if bq is not None and j in at:
                top = scores(bq, sq, at.index(j), 2 * w, top)
            if bv is not None and j < tiles:
                c = cbuf.at[bv % SLOTS]
                for h in range(chains):
                    t = lax.dot_general(c[r * h:r * (h + 1), w * j:w * (j + 1)], pb[:, w * j:w * (j + 1)], NT,
                                        preferred_element_type=jnp.float32)
                    acc[h] = t if j == 0 else acc[h] + t
        if bv is not None:
            for h in range(chains):
                obuf[bv + 1, :, r * h:r * (h + 1)] = (acc[h].T * inv).astype(jnp.bfloat16)
        if bq is not None:
            mxq[...] = top

    lbuf[...] = jnp.zeros_like(lbuf)
    lens.wait()
    forward_q(0)
    mate_copy(1, d, mate).start()
    cache_copy(2).start()
    cache_copy(3).start()
    mate_copy(0, mate, mate).wait_recv()
    cache_copy(0).wait()
    cache_copy(1).wait()
    wait_q(0)
    step(0, s_a, mx_a, None, None, None)
    forward_q(1)
    cache_copy(4).start()
    cache_copy(5).start()
    step(1, s_b, mx_b, 0, s_a, mx_a)
    mate_copy(1, mate, mate).wait_recv()

    def enter(k):
        if not isinstance(k, int):
            @pl.when(k < pairs - 1)
            def _():
                forward_q(k + 1)

        wait_q(k)
        if not isinstance(k, int):
            @pl.when(k < pairs - LEAD + 1)
            def _():
                q_copy(0, k + LEAD - 1, d, over).start()

            @pl.when(k < pairs - 2)
            def _():
                cache_copy(2 * k + 4).start()
                cache_copy(2 * k + 5).start()

            @pl.when(k == 1)
            def _():
                send_o(0)

            @pl.when(k > 1)
            def _():
                send_o(k - 1)
        else:
            send_o(k - 1)

        cache_copy(2 * k).wait()
        cache_copy(2 * k + 1).wait()

    def first(k):
        step(2 * k, s_a, mx_a, 2 * k - 1, s_b, mx_b)

    def second(k):
        step(2 * k + 1, s_b, mx_b, 2 * k, s_a, mx_a, at=(0, 2, 4, 8))

    def body(k, _):
        enter(k)
        first(k)
        second(k)
        return 0

    lax.fori_loop(1, pairs - 1, body, 0)

    def send_l():
        for i in (1, 2, 0):
            l_copy(i, d, peers[i]).start()

    enter(pairs - 1)
    first(pairs - 1)
    send_o(pairs - 1)
    second(pairs - 1)
    send_o(pairs)
    step(None, None, None, nb - 1, s_b, mx_b, known=send_l)
    send_o(pairs + 1)

    def shares():
        for i in (0, 1, 2):
            l_copy(i, peers[i], d).wait_recv()
        lses = [lbuf[rows(d), :]] + [lrecv[p] for p in peers]
        top = functools.reduce(jnp.maximum, lses)
        ws = [jnp.exp(x - top) for x in lses]
        norm = 1.0 / functools.reduce(jnp.add, ws)
        return [x * norm for x in ws]

    def merge(ws, b):
        lane = lax.broadcasted_iota(jnp.int32, ws[0].shape, 1)
        parts = [obuf[b + 1, rows(d), :]] + [orecv[p, b + 1] for p in peers]
        total = None
        for w, o in zip(ws, parts):
            col = jnp.sum(jnp.where(lane == b, w, 0.0), axis=1, keepdims=True)
            term = col * o.astype(jnp.float32)
            total = term if total is None else total + term
        out_ref[b] = total.astype(jnp.bfloat16)

    early = shares()
    wait_o(0)
    group = 6

    def merge_early(k, _):
        for r in range(group // 2):
            wait_o(group // 2 * k + r + 1)
        for r in range(group):
            merge(early, group * k + r)
        return 0

    whole = (nb - 3) // group
    lax.fori_loop(0, whole, merge_early, 0)
    for c in range(group // 2 * whole + 1, pairs - 1):
        wait_o(c)
    for b in range(group * whole, nb - 3):
        merge(early, b)
    for b in (nb - 3, nb - 2):
        wait_o(b - pairs + 2)
        merge(early, b)
    def drain(c, _):
        for i in (0, 1, 2):
            o_copy(i, c, d, peers[i]).wait_send()
        return 0

    lax.fori_loop(1, pairs - 1, drain, 0)
    for c in (0, pairs - 1, pairs):
        drain(c, 0)

    def drain_q(c, _):
        q_copy(0, c, d, over).wait_send()
        q_copy(1, c, over, mate).wait_send()
        return 0

    lax.fori_loop(0, pairs, drain_q, 0)
    for i in (0, 1):
        mate_copy(i, d, mate).wait_send()
    for i in (0, 1, 2):
        l_copy(i, d, peers[i]).wait_send()

    wait_o(pairs + 1)
    merge(early, nb - 1)
    drain(pairs + 1, 0)


def solution(mesh):
    n = mesh.shape['dcp']

    def local(q, cache, lengths):
        b, own, wd = q.shape
        sl = cache.shape[1]
        lat = wd - ROPE
        heads = own * n
        vmem = pl.BlockSpec(memory_space=pltpu.VMEM)
        return pl.pallas_call(
            kernel,
            out_shape=jax.ShapeDtypeStruct((b, own, lat), jnp.bfloat16),
            in_specs=[
                pl.BlockSpec(memory_space=pltpu.HBM),
                pl.BlockSpec(memory_space=pltpu.HBM),
                pl.BlockSpec(memory_space=pltpu.HBM),
            ],
            out_specs=vmem,
            scratch_shapes=[
                pltpu.VMEM((SLOTS, wd, sl), jnp.bfloat16),
                pltpu.VMEM((b, heads, wd), jnp.bfloat16),
                pltpu.VMEM((heads, sl), jnp.float32),
                pltpu.VMEM((heads, sl), jnp.float32),
                pltpu.VMEM((heads, 128), jnp.float32),
                pltpu.VMEM((heads, 128), jnp.float32),
                pltpu.VMEM((b + 2, heads, lat), jnp.bfloat16),
                pltpu.VMEM((n, b + 2, own, lat), jnp.bfloat16),
                pltpu.VMEM((heads, 128), jnp.float32),
                pltpu.VMEM((n, own, 128), jnp.float32),
                pltpu.SMEM((b,), jnp.int32),
                pltpu.SemaphoreType.DMA,
                pltpu.SemaphoreType.DMA((SLOTS,)),
                pltpu.SemaphoreType.DMA,
                pltpu.SemaphoreType.DMA((2,)),
                pltpu.SemaphoreType.DMA((2,)),
                pltpu.SemaphoreType.DMA((2, b // 2)),
                pltpu.SemaphoreType.DMA((2, b // 2)),
                pltpu.SemaphoreType.DMA((3, b // 2 + 2)),
                pltpu.SemaphoreType.DMA((3, b // 2 + 2)),
                pltpu.SemaphoreType.DMA((3,)),
                pltpu.SemaphoreType.DMA((3,)),
            ],
            compiler_params=pltpu.CompilerParams(
                collective_id=0, has_side_effects=True, vmem_limit_bytes=40 * 2 ** 20
            ),
            name='mla_decode',
        )(pltpu.with_memory_space_constraint(lengths, pltpu.HBM), pltpu.with_memory_space_constraint(q, pltpu.HBM), jnp.swapaxes(cache, 1, 2))

    return jax.shard_map(local, mesh=mesh, in_specs=(P('dp', 'dcp', None), P('dp', 'dcp', None), P('dp')), out_specs=P('dp', 'dcp', None), check_vma=False)
```

```python
import functools

import jax
import jax.numpy as jnp
from jax import lax
from jax.experimental import pallas as pl
from jax.experimental.pallas import tpu as pltpu
from jax.sharding import PartitionSpec as P

ROPE = 64
SCALE = 192 ** -0.5
LOG2E = 1.4426950408889634
SLOTS = 12
LEAD = 7
NT = (((1,), (1,)), ((), ()))


def kernel(lens_ref, q_ref, cache_ref, out_ref, cbuf, qbuf, s_a, s_b, mx_a, mx_b, obuf, orecv, lbuf, lrecv, len_ref,
           n_sem, c_sem, q_sem, ms_sem, mr_sem, qs_sem, qr_sem, os_sem, or_sem, ls_sem, lr_sem):
    nb, heads, wd = qbuf.shape
    own = q_ref.shape[1]
    lat = wd - ROPE
    sl = cbuf.shape[2]
    pairs = nb // 2
    g = lax.axis_index('dp')
    d = lax.axis_index('dcp')
    mate = d + 1 - 2 * (d % 2)
    over = (d + 2) % 4
    far = mate + 2 - 4 * (mate // 2)
    peers = (mate, over, far)

    def rows(j):
        return pl.ds(pl.multiple_of(j * own, own), own)

    def cache_copy(b):
        slot = b % SLOTS
        return pltpu.make_async_copy(cache_ref.at[b], cbuf.at[slot], c_sem.at[slot])

    def remote(src, dst, ssem, rsem, dev):
        return pltpu.make_async_remote_copy(src_ref=src, dst_ref=dst, send_sem=ssem, recv_sem=rsem,
                                            device_id=(g, dev), device_id_type=pl.DeviceIdType.MESH)

    def mate_copy(i, src_dev, to):
        view = qbuf.at[pl.ds(0, 2) if i == 0 else pl.ds(2, nb - 2), rows(src_dev), :]
        return remote(view, view, ms_sem.at[i], mr_sem.at[i], to)

    def q_copy(kind, c, src_dev, to):
        view = qbuf.at[pl.ds(2 * c, 2), rows(src_dev), :]
        return remote(view, view, qs_sem.at[kind, c], qr_sem.at[kind, c], to)

    def o_copy(i, c, src_dev, dst_dev):
        if isinstance(c, int) and (c == 0 or c >= pairs - 1):
            at = pl.ds(1 if c == 0 else c + pairs - 1, 1)
        else:
            at = pl.ds(2 * c, 2)
        return remote(obuf.at[at, rows(dst_dev), :], orecv.at[src_dev, at], os_sem.at[i, c], or_sem.at[i, c], dst_dev)

    def l_copy(i, src_dev, dst_dev):
        return remote(lbuf.at[rows(dst_dev), :], lrecv.at[src_dev], ls_sem.at[i], lr_sem.at[i], dst_dev)

    q_own = pltpu.make_async_copy(q_ref, qbuf.at[:, rows(d), :], q_sem)
    q_own.start()
    lens = pltpu.make_async_copy(lens_ref, len_ref, n_sem)
    lens.start()

    barrier = pltpu.get_barrier_semaphore()
    for p in peers:
        pl.semaphore_signal(barrier, inc=1, device_id=(g, p), device_id_type=pl.DeviceIdType.MESH)
    pl.semaphore_wait(barrier, 3)

    q_own.wait()
    q_copy(0, 0, d, over).start()
    mate_copy(0, d, mate).start()
    cache_copy(0).start()
    for c in range(1, LEAD):
        q_copy(0, c, d, over).start()
    cache_copy(1).start()

    def forward_q(c):
        q_copy(0, c, over, over).wait_recv()
        q_copy(1, c, over, mate).start()

    def wait_q(c):
        q_copy(1, c, far, mate).wait_recv()

    def send_o(c):
        for i in (1, 2, 0):
            o_copy(i, c, d, peers[i]).start()

    def wait_o(c):
        for i in (0, 1, 2):
            o_copy(i, c, peers[i], d).wait_recv()

    def scores(b, s_ref, j, w, top):
        n_valid = len_ref[b] - d * sl
        c = cbuf.at[b % SLOTS]
        s = jnp.dot(qbuf[b], c[:, w * j:w * (j + 1)], preferred_element_type=jnp.float32)
        pos = lax.broadcasted_iota(jnp.int32, s.shape, 1) + w * j
        s = jnp.where(pos < n_valid, s, -jnp.inf)
        s_ref[:, w * j:w * (j + 1)] = s
        for k in range(w // 128):
            t = s[:, 128 * k:128 * (k + 1)]
            top = t if top is None else jnp.maximum(top, t)
        return top

    def weights(b, s_ref, mx_ref):
        m = jnp.max(mx_ref[...], axis=1, keepdims=True)
        m0 = jnp.where(m == -jnp.inf, 0.0, m)
        p = jnp.exp2((s_ref[...] - m0) * (SCALE * LOG2E))
        l = jnp.sum(p, axis=1, keepdims=True)
        has = l > 0.0
        l1 = jnp.where(has, l, 1.0)
        lse = jnp.where(has, m0 * SCALE + jnp.log(l1), -jnp.inf)
        lane = lax.broadcasted_iota(jnp.int32, lbuf.shape, 1)
        lbuf[...] = jnp.where(lane == b, lse, lbuf[...])
        return p.astype(jnp.bfloat16), 1.0 / l1

    def step(bq, sq, mxq, bv, sv, mxv, at=(0, 2, 4, 6), known=None):
        tiles, chains = 8, 4
        w, r = sl // tiles, lat // chains
        if bv is not None:
            pb, inv = weights(bv, sv, mxv)
            if known is not None:
                known()
        top = None
        acc = [None] * chains
        for j in range(tiles + 1):
            if bq is not None and j in at:
                top = scores(bq, sq, at.index(j), 2 * w, top)
            if bv is not None and j < tiles:
                c = cbuf.at[bv % SLOTS]
                for h in range(chains):
                    t = lax.dot_general(c[r * h:r * (h + 1), w * j:w * (j + 1)], pb[:, w * j:w * (j + 1)], NT,
                                        preferred_element_type=jnp.float32)
                    acc[h] = t if j == 0 else acc[h] + t
        if bv is not None:
            for h in range(chains):
                obuf[bv + 1, :, r * h:r * (h + 1)] = (acc[h].T * inv).astype(jnp.bfloat16)
        if bq is not None:
            mxq[...] = top

    lbuf[...] = jnp.zeros_like(lbuf)
    lens.wait()
    forward_q(0)
    mate_copy(1, d, mate).start()
    cache_copy(2).start()
    cache_copy(3).start()
    mate_copy(0, mate, mate).wait_recv()
    cache_copy(0).wait()
    cache_copy(1).wait()
    wait_q(0)
    step(0, s_a, mx_a, None, None, None)
    forward_q(1)
    cache_copy(4).start()
    cache_copy(5).start()
    step(1, s_b, mx_b, 0, s_a, mx_a)
    mate_copy(1, mate, mate).wait_recv()

    def pair_starts(p):
        cache_copy(2 * p).start()
        cache_copy(2 * p + 1).start()

    def pair_waits(p):
        wait_q(p)
        cache_copy(2 * p).wait()
        cache_copy(2 * p + 1).wait()

    def send_q(c):
        q_copy(0, c, d, over).start()

    inner, outer = (0, 2, 4, 6), (0, 2, 4, 8)

    def first(k):
        step(2 * k, s_a, mx_a, 2 * k - 1, s_b, mx_b, at=inner)

    def second(k, at=outer):
        step(2 * k + 1, s_b, mx_b, 2 * k, s_a, mx_a, at=at)

    def opening(k, _):
        forward_q(k + 1)
        send_q(k + LEAD - 1)

        @pl.when(k == 1)
        def _():
            send_o(0)

        @pl.when(k == 2)
        def _():
            forward_q(4)
            send_q(LEAD + 2)
            send_o(1)

        pair_starts(k + 2)
        pair_waits(k)
        first(k)
        second(k)
        return 0

    lax.fori_loop(1, 3, opening, 0)

    def middle(t, _):
        k = 2 * t + 1
        forward_q(k + 2)
        forward_q(k + 3)

        @pl.when(k + LEAD + 1 < pairs)
        def _():
            send_q(k + LEAD)
            send_q(k + LEAD + 1)

        @pl.when(t > 1)
        def _():
            send_o(k - 2)

        send_o(k - 1)
        pair_starts(k + 2)
        pair_starts(k + 3)
        pair_waits(k)
        pair_waits(k + 1)
        first(k)
        second(k, inner)
        first(k + 1)
        second(k + 1)
        return 0

    lax.fori_loop(1, pairs // 2 - 2, middle, 0)

    def closing(k, _):
        @pl.when(k == pairs - 3)
        def _():
            forward_q(pairs - 1)
            pair_starts(pairs - 1)
            send_o(pairs - 5)

        send_o(k - 1)
        pair_waits(k)
        first(k)
        second(k)
        return 0

    lax.fori_loop(pairs - 3, pairs - 1, closing, 0)

    def send_l():
        for i in (1, 2, 0):
            l_copy(i, d, peers[i]).start()

    send_o(pairs - 2)
    pair_waits(pairs - 1)
    first(pairs - 1)
    send_o(pairs - 1)
    second(pairs - 1)
    send_o(pairs)
    step(None, None, None, nb - 1, s_b, mx_b, known=send_l)
    send_o(pairs + 1)

    def shares():
        for i in (0, 1, 2):
            l_copy(i, peers[i], d).wait_recv()
        lses = [lbuf[rows(d), :]] + [lrecv[p] for p in peers]
        top = functools.reduce(jnp.maximum, lses)
        ws = [jnp.exp(x - top) for x in lses]
        norm = 1.0 / functools.reduce(jnp.add, ws)
        return [x * norm for x in ws]

    def merge(ws, b):
        lane = lax.broadcasted_iota(jnp.int32, ws[0].shape, 1)
        parts = [obuf[b + 1, rows(d), :]] + [orecv[p, b + 1] for p in peers]
        total = None
        for w, o in zip(ws, parts):
            col = jnp.sum(jnp.where(lane == b, w, 0.0), axis=1, keepdims=True)
            term = col * o.astype(jnp.float32)
            total = term if total is None else total + term
        out_ref[b] = total.astype(jnp.bfloat16)

    early = shares()
    wait_o(0)
    group = 6

    def merge_early(k, _):
        for r in range(group // 2):
            wait_o(group // 2 * k + r + 1)
        for r in range(group):
            merge(early, group * k + r)
        return 0

    whole = (nb - 3) // group
    lax.fori_loop(0, whole, merge_early, 0)
    for c in range(group // 2 * whole + 1, pairs - 1):
        wait_o(c)
    for b in range(group * whole, nb - 3):
        merge(early, b)
    for b in (nb - 3, nb - 2):
        wait_o(b - pairs + 2)
        merge(early, b)
    def drain(c, _):
        for i in (0, 1, 2):
            o_copy(i, c, d, peers[i]).wait_send()
        return 0

    lax.fori_loop(1, pairs - 1, drain, 0)
    for c in (0, pairs - 1, pairs):
        drain(c, 0)

    def drain_q(c, _):
        q_copy(0, c, d, over).wait_send()
        q_copy(1, c, over, mate).wait_send()
        return 0

    lax.fori_loop(0, pairs, drain_q, 0)
    for i in (0, 1):
        mate_copy(i, d, mate).wait_send()
    for i in (0, 1, 2):
        l_copy(i, d, peers[i]).wait_send()

    wait_o(pairs + 1)
    merge(early, nb - 1)
    drain(pairs + 1, 0)


def solution(mesh):
    n = mesh.shape['dcp']

    def local(q, cache, lengths):
        b, own, wd = q.shape
        sl = cache.shape[1]
        lat = wd - ROPE
        heads = own * n
        vmem = pl.BlockSpec(memory_space=pltpu.VMEM)
        return pl.pallas_call(
            kernel,
            out_shape=jax.ShapeDtypeStruct((b, own, lat), jnp.bfloat16),
            in_specs=[
                pl.BlockSpec(memory_space=pltpu.HBM),
                pl.BlockSpec(memory_space=pltpu.HBM),
                pl.BlockSpec(memory_space=pltpu.HBM),
            ],
            out_specs=vmem,
            scratch_shapes=[
                pltpu.VMEM((SLOTS, wd, sl), jnp.bfloat16),
                pltpu.VMEM((b, heads, wd), jnp.bfloat16),
                pltpu.VMEM((heads, sl), jnp.float32),
                pltpu.VMEM((heads, sl), jnp.float32),
                pltpu.VMEM((heads, 128), jnp.float32),
                pltpu.VMEM((heads, 128), jnp.float32),
                pltpu.VMEM((b + 2, heads, lat), jnp.bfloat16),
                pltpu.VMEM((n, b + 2, own, lat), jnp.bfloat16),
                pltpu.VMEM((heads, 128), jnp.float32),
                pltpu.VMEM((n, own, 128), jnp.float32),
                pltpu.SMEM((b,), jnp.int32),
                pltpu.SemaphoreType.DMA,
                pltpu.SemaphoreType.DMA((SLOTS,)),
                pltpu.SemaphoreType.DMA,
                pltpu.SemaphoreType.DMA((2,)),
                pltpu.SemaphoreType.DMA((2,)),
                pltpu.SemaphoreType.DMA((2, b // 2)),
                pltpu.SemaphoreType.DMA((2, b // 2)),
                pltpu.SemaphoreType.DMA((3, b // 2 + 2)),
                pltpu.SemaphoreType.DMA((3, b // 2 + 2)),
                pltpu.SemaphoreType.DMA((3,)),
                pltpu.SemaphoreType.DMA((3,)),
            ],
            compiler_params=pltpu.CompilerParams(
                collective_id=0, has_side_effects=True, vmem_limit_bytes=46 * 2 ** 20
            ),
            name='mla_decode',
        )(pltpu.with_memory_space_constraint(lengths, pltpu.HBM), pltpu.with_memory_space_constraint(q, pltpu.HBM), jnp.swapaxes(cache, 1, 2))

    return jax.shard_map(local, mesh=mesh, in_specs=(P('dp', 'dcp', None), P('dp', 'dcp', None), P('dp')), out_specs=P('dp', 'dcp', None), check_vma=False)
```

```python
import functools

import jax
import jax.numpy as jnp
from jax import lax
from jax.experimental import pallas as pl
from jax.experimental.pallas import tpu as pltpu
from jax.sharding import PartitionSpec as P

ROPE = 64
SCALE = 192 ** -0.5
LOG2E = 1.4426950408889634
SLOTS = 12
LEAD = 7
NT = (((1,), (1,)), ((), ()))


def kernel(lens_ref, q_ref, cache_ref, out_ref, cbuf, qbuf, s_a, s_b, mx_a, mx_b, obuf, orecv, lbuf, lrecv, len_ref,
           n_sem, c_sem, q_sem, ms_sem, mr_sem, qs_sem, qr_sem, os_sem, or_sem, ls_sem, lr_sem):
    nb, heads, wd = qbuf.shape
    own = q_ref.shape[1]
    lat = wd - ROPE
    sl = cbuf.shape[2]
    pairs = nb // 2
    g = lax.axis_index('dp')
    d = lax.axis_index('dcp')
    mate = d + 1 - 2 * (d % 2)
    over = (d + 2) % 4
    far = mate + 2 - 4 * (mate // 2)
    peers = (mate, over, far)

    def rows(j):
        return pl.ds(pl.multiple_of(j * own, own), own)

    def cache_copy(b):
        slot = b % SLOTS
        return pltpu.make_async_copy(cache_ref.at[b], cbuf.at[slot], c_sem.at[slot])

    def remote(src, dst, ssem, rsem, dev):
        return pltpu.make_async_remote_copy(src_ref=src, dst_ref=dst, send_sem=ssem, recv_sem=rsem,
                                            device_id=(g, dev), device_id_type=pl.DeviceIdType.MESH)

    def mate_copy(i, src_dev, to):
        view = qbuf.at[pl.ds(0, 2) if i == 0 else pl.ds(2, nb - 2), rows(src_dev), :]
        return remote(view, view, ms_sem.at[i], mr_sem.at[i], to)

    def q_copy(kind, c, src_dev, to):
        if isinstance(c, int) and c in (0, pairs):
            at = pl.ds(0 if c == 0 else 1, 1)
        else:
            at = pl.ds(2 * c, 2)
        view = qbuf.at[at, rows(src_dev), :]
        return remote(view, view, qs_sem.at[kind, c], qr_sem.at[kind, c], to)

    def o_copy(i, c, src_dev, dst_dev):
        if isinstance(c, int) and (c == 0 or c >= pairs - 1):
            at = pl.ds(1 if c == 0 else c + pairs - 1, 1)
        else:
            at = pl.ds(2 * c, 2)
        return remote(obuf.at[at, rows(dst_dev), :], orecv.at[src_dev, at], os_sem.at[i, c], or_sem.at[i, c], dst_dev)

    def l_copy(i, src_dev, dst_dev):
        return remote(lbuf.at[rows(dst_dev), :], lrecv.at[src_dev], ls_sem.at[i], lr_sem.at[i], dst_dev)

    q_own = [pltpu.make_async_copy(q_ref.at[at], qbuf.at[at, rows(d), :], q_sem.at[i])
             for i, at in enumerate((pl.ds(0, 2), pl.ds(2, nb - 2)))]
    for copy in q_own:
        copy.start()
    lens = pltpu.make_async_copy(lens_ref, len_ref, n_sem)
    lens.start()

    barrier = pltpu.get_barrier_semaphore()
    for p in peers:
        pl.semaphore_signal(barrier, inc=1, device_id=(g, p), device_id_type=pl.DeviceIdType.MESH)
    pl.semaphore_wait(barrier, 3)

    q_own[0].wait()
    q_copy(0, 0, d, over).start()
    q_copy(0, pairs, d, over).start()
    mate_copy(0, d, mate).start()
    cache_copy(0).start()
    q_own[1].wait()
    for c in range(1, LEAD):
        q_copy(0, c, d, over).start()
    cache_copy(1).start()

    def forward_q(c):
        q_copy(0, c, over, over).wait_recv()
        q_copy(1, c, over, mate).start()

    def wait_q(c):
        q_copy(1, c, far, mate).wait_recv()

    def send_o(c):
        for i in (1, 2, 0):
            o_copy(i, c, d, peers[i]).start()

    def wait_o(c):
        for i in (0, 1, 2):
            o_copy(i, c, peers[i], d).wait_recv()

    def scores(b, s_ref, j, w, top):
        n_valid = len_ref[b] - d * sl
        c = cbuf.at[b % SLOTS]
        s = jnp.dot(qbuf[b], c[:, w * j:w * (j + 1)], preferred_element_type=jnp.float32)
        pos = lax.broadcasted_iota(jnp.int32, s.shape, 1) + w * j
        s = jnp.where(pos < n_valid, s, -jnp.inf)
        s_ref[:, w * j:w * (j + 1)] = s
        for k in range(w // 128):
            t = s[:, 128 * k:128 * (k + 1)]
            top = t if top is None else jnp.maximum(top, t)
        return top

    def weights(b, s_ref, mx_ref):
        m = jnp.max(mx_ref[...], axis=1, keepdims=True)
        m0 = jnp.where(m == -jnp.inf, 0.0, m)
        p = jnp.exp2((s_ref[...] - m0) * (SCALE * LOG2E))
        l = jnp.sum(p, axis=1, keepdims=True)
        has = l > 0.0
        l1 = jnp.where(has, l, 1.0)
        lse = jnp.where(has, m0 * SCALE + jnp.log(l1), -jnp.inf)
        lane = lax.broadcasted_iota(jnp.int32, lbuf.shape, 1)
        lbuf[...] = jnp.where(lane == b, lse, lbuf[...])
        return p.astype(jnp.bfloat16), 1.0 / l1

    def step(bq, sq, mxq, bv, sv, mxv, at=(0, 2, 4, 6), known=None):
        tiles, chains = 8, 4
        w, r = sl // tiles, lat // chains
        if bv is not None:
            pb, inv = weights(bv, sv, mxv)
            if known is not None:
                known()
        top = None
        acc = [None] * chains
        for j in range(tiles + 1):
            if bq is not None and j in at:
                top = scores(bq, sq, at.index(j), 2 * w, top)
            if bv is not None and j < tiles:
                c = cbuf.at[bv % SLOTS]
                for h in range(chains):
                    t = lax.dot_general(c[r * h:r * (h + 1), w * j:w * (j + 1)], pb[:, w * j:w * (j + 1)], NT,
                                        preferred_element_type=jnp.float32)
                    acc[h] = t if j == 0 else acc[h] + t
        if bv is not None:
            for h in range(chains):
                obuf[bv + 1, :, r * h:r * (h + 1)] = (acc[h].T * inv).astype(jnp.bfloat16)
        if bq is not None:
            mxq[...] = top

    lbuf[...] = jnp.zeros_like(lbuf)
    lens.wait()
    forward_q(0)
    forward_q(pairs)
    mate_copy(1, d, mate).start()
    cache_copy(2).start()
    cache_copy(3).start()
    mate_copy(0, mate, mate).wait_recv()
    cache_copy(0).wait()
    cache_copy(1).wait()
    wait_q(0)
    step(0, s_a, mx_a, None, None, None)
    wait_q(pairs)
    forward_q(1)
    cache_copy(4).start()
    cache_copy(5).start()
    step(1, s_b, mx_b, 0, s_a, mx_a)
    mate_copy(1, mate, mate).wait_recv()

    def pair_starts(p):
        cache_copy(2 * p).start()
        cache_copy(2 * p + 1).start()

    def pair_waits(p):
        wait_q(p)
        cache_copy(2 * p).wait()
        cache_copy(2 * p + 1).wait()

    def send_q(c):
        q_copy(0, c, d, over).start()

    inner, outer = (0, 2, 4, 6), (0, 2, 4, 8)

    def first(k):
        step(2 * k, s_a, mx_a, 2 * k - 1, s_b, mx_b, at=inner)

    def second(k, at=outer):
        step(2 * k + 1, s_b, mx_b, 2 * k, s_a, mx_a, at=at)

    def opening(k, _):
        forward_q(k + 1)
        send_q(k + LEAD - 1)

        @pl.when(k == 1)
        def _():
            send_o(0)

        @pl.when(k == 2)
        def _():
            forward_q(4)
            send_q(LEAD + 2)
            send_o(1)

        pair_starts(k + 2)
        pair_waits(k)
        first(k)
        second(k)
        return 0

    lax.fori_loop(1, 3, opening, 0)

    def middle(t, _):
        k = 2 * t + 1
        forward_q(k + 2)
        forward_q(k + 3)

        @pl.when(k + LEAD + 1 < pairs)
        def _():
            send_q(k + LEAD)
            send_q(k + LEAD + 1)

        @pl.when(t > 1)
        def _():
            send_o(k - 2)

        send_o(k - 1)
        pair_starts(k + 2)
        pair_starts(k + 3)
        pair_waits(k)
        pair_waits(k + 1)
        first(k)
        second(k, inner)
        first(k + 1)
        second(k + 1)
        return 0

    lax.fori_loop(1, pairs // 2 - 2, middle, 0)

    def closing(k, _):
        @pl.when(k == pairs - 3)
        def _():
            forward_q(pairs - 1)
            pair_starts(pairs - 1)
            send_o(pairs - 5)

        send_o(k - 1)
        pair_waits(k)
        first(k)
        second(k)
        return 0

    lax.fori_loop(pairs - 3, pairs - 1, closing, 0)

    def send_l():
        for i in (1, 2, 0):
            l_copy(i, d, peers[i]).start()

    send_o(pairs - 2)
    pair_waits(pairs - 1)
    first(pairs - 1)
    send_o(pairs - 1)
    second(pairs - 1)
    send_o(pairs)
    step(None, None, None, nb - 1, s_b, mx_b, known=send_l)
    send_o(pairs + 1)

    def shares():
        for i in (0, 1, 2):
            l_copy(i, peers[i], d).wait_recv()
        lses = [lbuf[rows(d), :]] + [lrecv[p] for p in peers]
        top = functools.reduce(jnp.maximum, lses)
        ws = [jnp.exp(x - top) for x in lses]
        norm = 1.0 / functools.reduce(jnp.add, ws)
        return [x * norm for x in ws]

    def merge(ws, b):
        lane = lax.broadcasted_iota(jnp.int32, ws[0].shape, 1)
        parts = [obuf[b + 1, rows(d), :]] + [orecv[p, b + 1] for p in peers]
        total = None
        for w, o in zip(ws, parts):
            col = jnp.sum(jnp.where(lane == b, w, 0.0), axis=1, keepdims=True)
            term = col * o.astype(jnp.float32)
            total = term if total is None else total + term
        out_ref[b] = total.astype(jnp.bfloat16)

    early = shares()
    wait_o(0)
    group = 6

    def merge_early(k, _):
        for r in range(group // 2):
            wait_o(group // 2 * k + r + 1)
        for r in range(group):
            merge(early, group * k + r)
        return 0

    whole = (nb - 3) // group
    lax.fori_loop(0, whole, merge_early, 0)
    for c in range(group // 2 * whole + 1, pairs - 1):
        wait_o(c)
    for b in range(group * whole, nb - 3):
        merge(early, b)
    for b in (nb - 3, nb - 2):
        wait_o(b - pairs + 2)
        merge(early, b)
    def drain(c, _):
        for i in (0, 1, 2):
            o_copy(i, c, d, peers[i]).wait_send()
        return 0

    lax.fori_loop(1, pairs - 1, drain, 0)
    for c in (0, pairs - 1, pairs):
        drain(c, 0)

    def drain_q(c, _):
        q_copy(0, c, d, over).wait_send()
        q_copy(1, c, over, mate).wait_send()
        return 0

    lax.fori_loop(1, pairs, drain_q, 0)
    for c in (0, pairs):
        drain_q(c, 0)
    for i in (0, 1):
        mate_copy(i, d, mate).wait_send()
    for i in (0, 1, 2):
        l_copy(i, d, peers[i]).wait_send()

    wait_o(pairs + 1)
    merge(early, nb - 1)
    drain(pairs + 1, 0)


def solution(mesh):
    n = mesh.shape['dcp']

    def local(q, cache, lengths):
        b, own, wd = q.shape
        sl = cache.shape[1]
        lat = wd - ROPE
        heads = own * n
        vmem = pl.BlockSpec(memory_space=pltpu.VMEM)
        return pl.pallas_call(
            kernel,
            out_shape=jax.ShapeDtypeStruct((b, own, lat), jnp.bfloat16),
            in_specs=[
                pl.BlockSpec(memory_space=pltpu.HBM),
                pl.BlockSpec(memory_space=pltpu.HBM),
                pl.BlockSpec(memory_space=pltpu.HBM),
            ],
            out_specs=vmem,
            scratch_shapes=[
                pltpu.VMEM((SLOTS, wd, sl), jnp.bfloat16),
                pltpu.VMEM((b, heads, wd), jnp.bfloat16),
                pltpu.VMEM((heads, sl), jnp.float32),
                pltpu.VMEM((heads, sl), jnp.float32),
                pltpu.VMEM((heads, 128), jnp.float32),
                pltpu.VMEM((heads, 128), jnp.float32),
                pltpu.VMEM((b + 2, heads, lat), jnp.bfloat16),
                pltpu.VMEM((n, b + 2, own, lat), jnp.bfloat16),
                pltpu.VMEM((heads, 128), jnp.float32),
                pltpu.VMEM((n, own, 128), jnp.float32),
                pltpu.SMEM((b,), jnp.int32),
                pltpu.SemaphoreType.DMA,
                pltpu.SemaphoreType.DMA((SLOTS,)),
                pltpu.SemaphoreType.DMA((2,)),
                pltpu.SemaphoreType.DMA((2,)),
                pltpu.SemaphoreType.DMA((2,)),
                pltpu.SemaphoreType.DMA((2, b // 2 + 1)),
                pltpu.SemaphoreType.DMA((2, b // 2 + 1)),
                pltpu.SemaphoreType.DMA((3, b // 2 + 2)),
                pltpu.SemaphoreType.DMA((3, b // 2 + 2)),
                pltpu.SemaphoreType.DMA((3,)),
                pltpu.SemaphoreType.DMA((3,)),
            ],
            compiler_params=pltpu.CompilerParams(
                collective_id=0, has_side_effects=True, vmem_limit_bytes=46 * 2 ** 20
            ),
            name='mla_decode',
        )(pltpu.with_memory_space_constraint(lengths, pltpu.HBM), pltpu.with_memory_space_constraint(q, pltpu.HBM), jnp.swapaxes(cache, 1, 2))

    return jax.shard_map(local, mesh=mesh, in_specs=(P('dp', 'dcp', None), P('dp', 'dcp', None), P('dp')), out_specs=P('dp', 'dcp', None), check_vma=False)
```
